32 devices in a mesh: seq: 8 (over z, x), head: 4 (over y, core).
Axes of the slice: x: 2, y: 2, z: 4, core: 2. Of those that a mesh axis runs over, the one named last changes fastest.
Arguments:
- queries: bfloat16 [4096, 6144], P('seq', 'head'), may hold values from -10 to 10
- keys: bfloat16 [4096, 6144], P('seq', 'head'), may hold values from -10 to 10
- values: bfloat16 [4096, 6144], P('seq', 'head'), may hold values from -6 to 6
- frame_of_block: int32 [16], P('seq'), may hold values from 0 to 7, never falling along the last dimension, each value on 1 to 4 neighbouring positions
- pair_mask: int32 [16, 16], P('seq'), may hold values 0 or 1
- w_out: bfloat16 [6144, 6144], P('head', 'seq'), may hold values from -0.4375 to 0.4375
Outputs:
- projected: bfloat16 [4096, 6144], P('seq', 'head')
The draws below stay inside these ranges and needn't reach their ends.
Inputs may be any that keep to these rules, and one draw needn't show every extreme that they name: `frame_of_block`: frame ids never fall along the blocks, every frame spans 1 to 4 consecutive blocks.
All inputs are finite; a program needn't handle non-finite values. No bound on the sum of `pair_mask` on one device may be relied on, other than what follows from the above.
Results may differ from the reference program's by a relative error of at most 0.015.
Values may be sent and summed in bfloat16 or wider, within the bound.
A program may use at most 192 MiB of HBM per device.

```python
import math
import jax
import jax.numpy as jnp
import numpy as np
from jax import lax

D = 6144
H = 48
HD = 128
BLK = 256
TOK_DEV = 512
TOKENS = 4096
NBLK = 16
FRAMES = 8


def joint_draw(key):
    width = H * HD
    q_draw = jnp.clip(1.5 * jax.random.normal(jax.random.fold_in(key, 101), (TOKENS, width), jnp.float32), -6.0, 6.0)
    k_draw = jnp.clip(1.5 * jax.random.normal(jax.random.fold_in(key, 202), (TOKENS, width), jnp.float32), -6.0, 6.0)
    return (q_draw, k_draw)


def draw_queries(key, part):
    return joint_draw(key)[0].astype(jnp.bfloat16)


def draw_keys(key, part):
    return joint_draw(key)[1].astype(jnp.bfloat16)


def touch_ends(result, stream_key, least, largest):
    spot = [jax.random.randint(jax.random.fold_in(stream_key, axis), (), 0, length) for axis, length in enumerate(result.shape)]
    main_axis = result.shape.index(max(result.shape))
    beside = spot[:main_axis] + [(spot[main_axis] + 1) % result.shape[main_axis]] + spot[main_axis + 1:]
    return result.at[tuple(spot)].set(least).at[tuple(beside)].set(largest)


def shard_levels(own_key, extent, shards, low, largest):
    factor_of, own = 1.0, jax.random.fold_in(own_key, 6)
    for dim, parts in shards:
        steps = jnp.exp(jax.random.uniform(jax.random.fold_in(own, dim), (parts,), jnp.float32, low / len(shards), largest / len(shards)))
        factor_of = factor_of * jnp.repeat(steps, extent[dim] // parts).reshape([-1 if axis == dim else 1 for axis in range(len(extent))])
    return factor_of


def length_profile(count, total, most, slope):
    weights = [(1 << 20) // math.isqrt(standing ** slope) + 1 for standing in range(2, count + 1)]
    spare, given = total - most - (count - 1), [1] * (count - 1)
    while spare > 0:
        movable = [i for i in range(count - 1) if given[i] < most]
        mass, left = sum([weights[i] for i in movable]), spare
        for i in movable:
            more = min(most - given[i], max(1, left * weights[i] // mass), spare)
            given[i] = given[i] + more
            spare = spare - more
    return np.array([most] + given)


def uneven_parts(key, amount, total, reach, skew):
    if amount == 2:
        one = jax.random.randint(key, (), max(1, total - reach), min(reach, total - 1) + 1)
        return jnp.stack([one, total - one])
    tallies = jnp.asarray(length_profile(amount, total, reach, skew), jnp.int32)
    twos = (amount - 1) // 2
    giver, sink = tallies[1:1 + 2 * twos:2], tallies[2:2 + 2 * twos:2]
    slack = jnp.minimum(giver - 1, reach - sink)
    shifted = jax.random.randint(jax.random.fold_in(key, 1), (twos,), 0, 1 << 20) % (slack + 1)
    tallies = tallies.at[1:1 + 2 * twos:2].set(giver - shifted).at[2:2 + 2 * twos:2].set(sink + shifted)
    return tallies[jax.random.permutation(jax.random.fold_in(key, 2), amount)]


def noise(stream_key, dims, scale, most, pieces=(), kind=jnp.bfloat16):
    values = scale * jax.random.normal(stream_key, dims, jnp.float32)
    if pieces:
        values = values * shard_levels(stream_key, dims, pieces, -0.22, 0.18)
    return jnp.clip(values, -most, most).astype(kind)


def setup_inputs(seed: int = 0) -> dict:
    key_of = jax.random.split(jax.random.key(seed), 7)
    return {
        "queries": draw_queries(jax.random.fold_in(key_of[6], 71), 0),
        "keys": draw_keys(jax.random.fold_in(key_of[6], 71), 0),
        "values": noise(key_of[2], (TOKENS, D), 1.0, 6.0, ((0, 8), (1, 4))),
        "frame_of_block": jnp.searchsorted(jnp.cumsum(uneven_parts(key_of[3], FRAMES, NBLK, 4, 1)), jnp.arange(NBLK), side="right").astype(jnp.int32),
        "pair_mask": touch_ends((jax.random.randint(key_of[4], (NBLK, NBLK), 0, 4) < 3).astype(jnp.int32), jax.random.fold_in(key_of[4], 1), 0, 1),
        "w_out": noise(key_of[5], (D, D), (D // 32) ** -0.5, 0.4375, ((0, 4), (1, 8))),
    }


def reference(queries, keys, values, frame_of_block, pair_mask, w_out):
    width = H * HD
    scale = 1.0 / math.sqrt(HD)
    tok_frame = jnp.repeat(frame_of_block, BLK)
    key_block = (jnp.arange(TOKENS, dtype=jnp.int32) // BLK).astype(jnp.int32)
    count_blocks = TOKENS // TOK_DEV

    def one_block(index):
        first = (index * TOK_DEV).astype(jnp.int32)
        rows = lax.dynamic_slice_in_dim(queries, first, TOK_DEV, 0)
        q_frame = lax.dynamic_slice_in_dim(tok_frame, first, TOK_DEV, 0)
        q_block = ((first + jnp.arange(TOK_DEV, dtype=jnp.int32)) // BLK).astype(jnp.int32)
        link = pair_mask[q_block][:, key_block]
        allowed = (tok_frame[None, :] <= q_frame[:, None]) & ((link == 1) | (tok_frame[None, :] == q_frame[:, None]))

        def one_head(head_index):
            col = (head_index * HD).astype(jnp.int32)
            q_head = lax.dynamic_slice_in_dim(rows, col, HD, 1)
            k_head = lax.dynamic_slice_in_dim(keys, col, HD, 1)
            v_head = lax.dynamic_slice_in_dim(values, col, HD, 1)
            score = jnp.dot(q_head, k_head.T, preferred_element_type=jnp.float32) * scale
            score = jnp.where(allowed, score, -1e+30)
            peak = lax.optimization_barrier(jnp.max(score, axis=1))
            weight = jnp.where(allowed, jnp.exp(score - peak[:, None]), 0.0)
            total = lax.optimization_barrier(jnp.sum(weight, axis=1))
            mixed = jnp.dot(weight.astype(jnp.bfloat16), v_head, preferred_element_type=jnp.float32)
            return mixed / total[:, None]
        heads = lax.map(one_head, jnp.arange(H, dtype=jnp.int32))
        return jnp.transpose(heads, (1, 0, 2)).reshape(TOK_DEV, width).astype(jnp.bfloat16)
    attn = lax.map(one_block, jnp.arange(count_blocks, dtype=jnp.int32)).reshape(TOKENS, width)
    return jnp.dot(attn, w_out, preferred_element_type=jnp.float32).astype(jnp.bfloat16)
```

```python
import functools
import math

import jax
import jax.numpy as jnp
from jax import lax
from jax.experimental import pallas as pl
from jax.experimental.pallas import tpu as pltpu
from jax.sharding import PartitionSpec as P

HD = 128
BLK = 256
NEG = -1e30
EARLY = 6


def body_gather(queries, keys, values, frame_of_block, pair_mask, w_out):
    tok = queries.shape[0]
    heads_here = queries.shape[1] // HD
    count_blocks = pair_mask.shape[1]
    scale = 1.0 / math.sqrt(HD)
    key_span = 512
    q_heads = queries.reshape(tok, heads_here, HD)
    q_frame = jnp.repeat(frame_of_block, BLK)
    mask_rows = jnp.repeat(pair_mask.astype(jnp.float32), BLK, axis=0)
    block_ids = jnp.arange(count_blocks, dtype=jnp.int32)

    def update(state, k_rows, v_rows, allowed):
        peak, total, accum = state
        k_heads = k_rows.reshape(k_rows.shape[0], heads_here, HD)
        v_heads = v_rows.reshape(v_rows.shape[0], heads_here, HD)
        score = (
            jnp.einsum("qhd,khd->hqk", q_heads, k_heads, preferred_element_type=jnp.float32) * scale
        )
        score = jnp.where(allowed[None], score, -1e30)
        new_peak = jnp.maximum(peak, jnp.max(score, axis=2))
        weight = jnp.where(allowed[None], jnp.exp(score - new_peak[:, :, None]), 0.0)
        factor = jnp.exp(peak - new_peak)
        new_total = total * factor + jnp.sum(weight, axis=2)
        added = jnp.einsum(
            "hqk,khd->qhd", weight.astype(jnp.bfloat16), v_heads, preferred_element_type=jnp.float32
        )
        new_accum = accum * factor.T[:, :, None] + added
        return (new_peak, new_total, new_accum)

    def attend_block(state, k_rows, v_rows, k_frame, start):
        count = k_rows.shape[0]
        k_block = (start + jnp.arange(count, dtype=jnp.int32)) // BLK
        one_hot = (block_ids[:, None] == k_block[None, :]).astype(jnp.float32)
        link = jnp.dot(mask_rows, one_hot, preferred_element_type=jnp.float32)
        same = k_frame[None, :] == q_frame[:, None]
        allowed = (k_frame[None, :] <= q_frame[:, None]) & ((link > 0.5) | same)
        return update(state, k_rows, v_rows, allowed)

    initial = (
        jnp.full((heads_here, tok), -1e30, jnp.float32),
        jnp.zeros((heads_here, tok), jnp.float32),
        jnp.zeros((tok, heads_here, HD), jnp.float32),
    )
    k_frame_local = jnp.repeat(frame_of_block, BLK)
    k_rows = lax.all_gather(keys, "seq", axis=0, tiled=True)
    v_rows = lax.all_gather(values, "seq", axis=0, tiled=True)
    k_frame = lax.all_gather(k_frame_local, "seq", axis=0, tiled=True)
    count = k_rows.shape[0]

    def step(index, inner):
        offset = (index * key_span).astype(jnp.int32)
        return attend_block(
            inner,
            lax.dynamic_slice_in_dim(k_rows, offset, key_span, 0),
            lax.dynamic_slice_in_dim(v_rows, offset, key_span, 0),
            lax.dynamic_slice_in_dim(k_frame, offset, key_span, 0),
            offset,
        )

    state = lax.fori_loop(0, count // key_span, step, initial)
    peak, total, accum = state
    attn = (accum / total.T[:, :, None]).reshape(tok, heads_here * HD).astype(jnp.bfloat16)
    terms = jnp.dot(
        attn, lax.all_gather(w_out, "seq", axis=1, tiled=True), preferred_element_type=jnp.float32
    )
    return lax.psum_scatter(terms.astype(jnp.bfloat16), "head", scatter_dimension=1, tiled=True)


def greet(n, me):
    barrier = pltpu.get_barrier_semaphore()
    for k in range(1, n):
        pl.semaphore_signal(barrier, inc=1, device_id={"seq": lax.rem(me + k, n)}, device_id_type=pl.DeviceIdType.MESH)
    pl.semaphore_wait(barrier, n - 1)


def cols(head):
    return pl.ds(pl.multiple_of(head * HD, HD), HD)


def rows(start, size):
    return pl.ds(pl.multiple_of(start, size), size)


def spread_kernel(n, tok, q, k, v, meta, qf, qs, kf, ks, vf, vs, metas, hold, hold_half, hold_meta, send, recv, here):
    me = lax.axis_index("seq")
    half = tok // 2

    def pieces(to):
        pair, odd = to // 2, lax.rem(to, 2)
        own, shared = cols(3 * pair + 2 * odd), cols(3 * pair + 1)
        full = rows(me * tok, tok)
        return [
            (meta, metas.at[rows(me * 8, 8)]),
            (q.at[:, own], qf.at[full]),
            (k.at[:, own], kf.at[full]),
            (v.at[:, own], vf.at[full]),
            (q.at[rows(odd * half, half), shared], qs.at[rows(me * half, half)]),
            (k.at[:, shared], ks.at[full]),
            (v.at[:, shared], vs.at[full]),
        ]

    def bounce(index):
        if index == 0:
            return hold_meta
        if index == 4:
            return hold_half
        return hold.at[{1: 0, 2: 1, 3: 2, 5: 3, 6: 4}[index]]

    greet(n, me)
    copies = []
    for step in range(1, n):
        to = lax.rem(me + step, n)
        for i, (src, dst) in enumerate(pieces(to)):
            copy = pltpu.make_async_remote_copy(
                src_ref=src, dst_ref=dst, send_sem=send.at[step - 1, i], recv_sem=recv.at[step - 1, i],
                device_id={"seq": to}, device_id_type=pl.DeviceIdType.MESH,
            )
            copy.start()
            copies.append(copy)
    mine = pieces(me)
    ins = [pltpu.make_async_copy(src, bounce(i), here.at[0, i]) for i, (src, _) in enumerate(mine)]
    outs = [pltpu.make_async_copy(bounce(i), dst, here.at[1, i]) for i, (_, dst) in enumerate(mine)]
    for c in ins:
        c.start()
    for c, d in zip(ins, outs):
        c.wait()
        d.start()
    for d in outs:
        d.wait()
    for c in copies:
        c.wait()


def project_kernel(
    n, tok, early, of, os, w, wgot, out, attn, wbuf, part, d_send, d_recv, y_send, y_recv, final,
    send1, recv1, here, send2, recv2, wsem_s, wsem_r, dsem_s, dsem_r, ysem_s, ysem_r, osem_s, osem_r,
):
    me, head = lax.axis_index("seq"), lax.axis_index("head")
    quad = n // 2
    half = tok // 2
    wide = w.shape[1]
    pair, odd = me // 2, lax.rem(me, 2)
    own, shared = cols(3 * pair + 2 * odd), cols(3 * pair + 1)
    c, y = lax.rem(head, 2), head // 2
    mine = me // quad
    x, zl = lax.rem(me, 2), lax.rem(me // 2, 2)
    base = mine * quad
    peers = [me, base + 2 * zl + 1 - x, base + 2 * (1 - zl) + x, base + 2 * (1 - zl) + 1 - x]
    partner = lax.rem(me + quad, n)
    core_peer = 2 * y + 1 - c
    y_peer = 2 * (1 - y) + c

    def remote(src, dst, send, recv, seq, hd):
        return pltpu.make_async_remote_copy(
            src_ref=src, dst_ref=dst, send_sem=send, recv_sem=recv,
            device_id={"seq": seq, "head": hd}, device_id_type=pl.DeviceIdType.MESH,
        )

    barrier = pltpu.get_barrier_semaphore()
    friends = [(lax.rem(me + k, n), head) for k in range(1, n)]
    friends += [(p, core_peer) for p in peers] + [(me, y_peer)]
    for seq, hd in friends:
        pl.semaphore_signal(barrier, inc=1, device_id={"seq": seq, "head": hd}, device_id_type=pl.DeviceIdType.MESH)
    own_w = pltpu.make_async_copy(w, wbuf.at[mine], here.at[2])
    own_w.start()
    got_w = pltpu.make_async_copy(wgot, wbuf.at[1 - mine, pl.ds(0, early)], here.at[3])
    got_w.start()
    pl.semaphore_wait(barrier, len(friends))

    def pieces(to):
        return [
            (of.at[rows(to * tok, tok)], attn.at[0, :, own]),
            (os.at[rows(to * half, half)], attn.at[0, rows(odd * half, half), shared]),
        ]

    back = []
    for step in range(1, n):
        to = lax.rem(me + step, n)
        for i, (src, dst) in enumerate(pieces(to)):
            copy = remote(src, dst, send1.at[step - 1, i], recv1.at[step - 1, i], to, head)
            copy.start()
            back.append(copy)
    local = [pltpu.make_async_copy(src, dst, here.at[i]) for i, (src, dst) in enumerate(pieces(me))]
    for copy in local:
        copy.start()
    for copy in local:
        copy.wait()
    for copy in back:
        copy.wait_send()
    w_copy = remote(
        w.at[pl.ds(early, w.shape[0] - early)], wbuf.at[mine, pl.ds(early, w.shape[0] - early)],
        wsem_s, wsem_r, partner, head,
    )
    for copy in back:
        copy.wait_recv()
    to_x = remote(attn.at[0], attn.at[1], send2.at[0], recv2.at[0], peers[1], head)
    to_z = remote(attn.at[0], attn.at[2], send2.at[1], recv2.at[1], peers[2], head)
    on_x = remote(attn.at[2], attn.at[3], send2.at[2], recv2.at[2], peers[1], head)
    to_z.start()
    to_x.start()
    w_copy.start()
    own_w.wait()

    def block_of(unit):
        return mine if unit < 4 else 1 - mine

    def swap(unit):
        return remote(d_send.at[unit], d_recv.at[unit], dsem_s.at[unit], dsem_r.at[unit], me, core_peer)

    def over_y(r):
        return remote(y_send.at[r], y_recv.at[r], ysem_s.at[r], ysem_r.at[r], me, y_peer)

    def home(r):
        dst = out.at[rows(c * half, half), pl.ds(pl.multiple_of(x * wide, HD), wide)]
        return remote(final.at[r], dst, osem_s.at[r], osem_r.at[2 * x + c], peers[r], 2 * y + zl)

    def home_here():
        dst = out.at[rows(c * half, half), pl.ds(pl.multiple_of(x * wide, HD), wide)]
        return pltpu.make_async_copy(final.at[0], dst, here.at[4])

    def multiply(unit):
        r, block = unit % 4, block_of(unit)

        def one(t, carry):
            side = (1 - c) * (1 - t) + c * t
            value = jnp.dot(attn[r, rows(side * half, half), :], wbuf[block], preferred_element_type=jnp.float32)

            @pl.when(t == 0)
            def _():
                d_send[unit] = value.astype(jnp.bfloat16)
                swap(unit).start()

            @pl.when(t == 1)
            def _():
                part[unit] = value

            return carry

        lax.fori_loop(0, 2, one, 0)

    def add_core(unit):
        r, block = unit % 4, block_of(unit)
        swap(unit).wait_recv()

        @pl.when(y == block)
        def _():
            part[unit] = part[unit] + d_recv[unit].astype(jnp.float32)

        @pl.when(y != block)
        def _():
            y_send[r] = (part[unit] + d_recv[unit].astype(jnp.float32)).astype(jnp.bfloat16)
            over_y(r).start()

    def finish(unit):
        r, block = unit % 4, block_of(unit)

        @pl.when(y == block)
        def _():
            over_y(r).wait_recv()
            final[r] = (part[unit] + y_recv[r].astype(jnp.float32)).astype(jnp.bfloat16)
            if r:
                home(r).start()
            else:
                @pl.when(zl != c)
                def _():
                    home(0).start()

                @pl.when(zl == c)
                def _():
                    home_here().start()

    multiply(0)
    to_z.wait_recv()
    on_x.start()
    to_x.wait_recv()
    multiply(1)
    add_core(0)
    multiply(2)
    add_core(1)
    finish(0)
    on_x.wait_recv()
    multiply(3)
    add_core(2)
    finish(1)
    add_core(3)
    finish(2)
    finish(3)
    got_w.wait()
    w_copy.wait_recv()
    multiply(4)
    multiply(5)
    add_core(4)
    multiply(6)
    add_core(5)
    multiply(7)
    add_core(6)
    add_core(7)
    for unit in range(4, 8):
        finish(unit)

    for copy in (to_x, to_z, on_x, w_copy):
        copy.wait_send()
    for unit in range(8):
        swap(unit).wait_send()
    for r in range(4):
        over_y(r).wait_send()
        if r:
            home(r).wait_send()

    @pl.when(zl != c)
    def _():
        home(0).wait_send()

    @pl.when(zl == c)
    def _():
        home_here().wait()

    for sx in range(2):
        for sc in range(2):
            piece = final.at[0]
            arrived = remote(piece, piece, osem_s.at[0], osem_r.at[2 * sx + sc], me, core_peer)

            @pl.when((zl != c) | (sx != x) | (sc != c))
            def _():
                arrived.wait_recv()


def attend_kernel(odd_ref, count_ref, list_ref, qf, qs, kf, ks, vf, vs, of, os):
    odd = odd_ref[0]
    j = pl.program_id(0)
    factor = math.log2(math.e) / math.sqrt(HD)

    def scores(q, k):
        return lax.dot_general(q, k, (((1,), (1,)), ((), ())), preferred_element_type=jnp.float32)

    def fold(state, parts, vals):
        peak, total, accum = state
        top = parts[0]
        for s in parts[1:]:
            top = jnp.maximum(top, s)
        new_peak = jnp.maximum(peak, jnp.max(top, axis=1, keepdims=True))
        keep = jnp.exp2((peak - new_peak) * factor)
        total, accum = total * keep, accum * keep
        for s, v in zip(parts, vals):
            p = jnp.exp2((s - new_peak) * factor)
            for c in range(0, BLK, HD):
                total = total + p[:, c:c + HD]
            accum = accum + jnp.dot(p.astype(jnp.bfloat16), v, preferred_element_type=jnp.float32)
        return new_peak, total, accum

    def start():
        return (
            jnp.full((BLK, 1), NEG, jnp.float32),
            jnp.zeros((BLK, HD), jnp.float32),
            jnp.zeros((BLK, HD), jnp.float32),
        )

    def finish(state):
        _, total, accum = state
        return (accum / jnp.sum(total, axis=1, keepdims=True)).astype(jnp.bfloat16)

    def walk(block, streams):
        count = count_ref[block]

        def step(i, states):
            a = rows(list_ref[block, 2 * i] * BLK, BLK)
            b = rows(list_ref[block, 2 * i + 1] * BLK, BLK)
            bias = jnp.where(2 * i + 1 < count, 0.0, NEG).astype(jnp.float32)
            parts = [[scores(q, k[a, :]), scores(q, k[b, :]) + bias] for q, k, _ in streams]
            return tuple(
                fold(state, part, (v[a, :], v[b, :])) for state, part, (_, _, v) in zip(states, parts, streams)
            )

        return lax.fori_loop(0, (count + 1) // 2, step, tuple(start() for _ in streams))

    same, other = rows(odd * BLK, BLK), rows((1 - odd) * BLK, BLK)
    first, second = walk(2 * j + odd, [(qf[same, :], kf, vf), (qs[...], ks, vs)])
    of[same, :] = finish(first)
    os[...] = finish(second)
    (third,) = walk(2 * j + 1 - odd, [(qf[other, :], kf, vf)])
    of[other, :] = finish(third)


def body_spread(n, queries, keys, values, frame_of_block, pair_mask, w_out):
    tok, width = queries.shape
    count_blocks = pair_mask.shape[1]
    tokens = n * tok
    per = tok // BLK
    meta = jnp.concatenate([frame_of_block[:, None], pair_mask], axis=1)
    meta = jnp.pad(meta, ((0, 8 - per), (0, HD - 1 - count_blocks)))
    anyspace = pl.BlockSpec(memory_space=pl.ANY)
    big = jax.ShapeDtypeStruct((tokens, HD), queries.dtype)
    small = jax.ShapeDtypeStruct((tokens // 2, HD), queries.dtype)
    qf, qs, kf, ks, vf, vs, metas = pl.pallas_call(
        functools.partial(spread_kernel, n, tok),
        out_shape=[big, small, big, big, big, big, jax.ShapeDtypeStruct((8 * n, HD), jnp.int32)],
        in_specs=[anyspace] * 4,
        out_specs=[anyspace] * 7,
        scratch_shapes=[
            pltpu.VMEM((5, tok, HD), queries.dtype),
            pltpu.VMEM((tok // 2, HD), queries.dtype),
            pltpu.VMEM((8, HD), jnp.int32),
            pltpu.SemaphoreType.DMA((n - 1, 7)),
            pltpu.SemaphoreType.DMA((n - 1, 7)),
            pltpu.SemaphoreType.DMA((2, 7)),
        ],
        compiler_params=pltpu.CompilerParams(collective_id=0, has_side_effects=True),
        cost_estimate=pl.CostEstimate(flops=0, bytes_accessed=300_000_000, transcendentals=0),
        name="spread",
    )(queries, keys, values, meta)

    metas = metas.reshape(n, 8, HD)[:, :per].reshape(n * per, HD)
    frame, links = metas[:, 0], metas[:, 1:1 + count_blocks]
    allowed = (frame[None, :] <= frame[:, None]) & ((links == 1) | (frame[None, :] == frame[:, None]))
    place = jnp.cumsum(allowed.astype(jnp.int32), axis=1)
    count = place[:, -1]
    ids = jnp.arange(count_blocks, dtype=jnp.int32)
    hit = allowed[:, None, :] & (place[:, None, :] == ids[None, :, None] + 1)
    order = jnp.sum(jnp.where(hit, ids[None, None, :], 0), axis=2)
    odd = lax.rem(lax.axis_index("seq"), 2).reshape(1).astype(jnp.int32)

    smem = pl.BlockSpec(memory_space=pltpu.SMEM)
    whole = pl.BlockSpec((tokens, HD), lambda j: (0, 0))
    two = pl.BlockSpec((2 * BLK, HD), lambda j: (j, 0))
    one = pl.BlockSpec((BLK, HD), lambda j: (j, 0))
    of, os = pl.pallas_call(
        attend_kernel,
        grid=(tokens // (2 * BLK),),
        out_shape=[big, small],
        in_specs=[smem, smem, smem, two, one, whole, whole, whole, whole],
        out_specs=[two, one],
        compiler_params=pltpu.CompilerParams(vmem_limit_bytes=48 * 1024 * 1024),
        cost_estimate=pl.CostEstimate(flops=20_000_000_000, bytes_accessed=8_000_000, transcendentals=20_000_000),
        name="attend",
    )(odd, count, order, qf, qs, kf, ks, vf, vs)

    quad = n // 2
    deep, wide = w_out.shape
    early = EARLY * deep // 16
    w_early, _ = lax.optimization_barrier((w_out[:early], kf))
    w_got = lax.ppermute(w_early, "seq", [(i, (i + quad) % n) for i in range(n)])
    dma = pltpu.SemaphoreType.DMA
    return pl.pallas_call(
        functools.partial(project_kernel, n, tok, early),
        out_shape=jax.ShapeDtypeStruct((tok, 2 * wide), queries.dtype),
        in_specs=[anyspace] * 4,
        out_specs=anyspace,
        scratch_shapes=[
            pltpu.VMEM((4, tok, width), queries.dtype),
            pltpu.VMEM((2, deep, wide), queries.dtype),
            pltpu.VMEM((8, tok // 2, wide), jnp.float32),
            pltpu.VMEM((8, tok // 2, wide), queries.dtype),
            pltpu.VMEM((8, tok // 2, wide), queries.dtype),
            pltpu.VMEM((4, tok // 2, wide), queries.dtype),
            pltpu.VMEM((4, tok // 2, wide), queries.dtype),
            pltpu.VMEM((4, tok // 2, wide), queries.dtype),
            dma((n - 1, 2)), dma((n - 1, 2)), dma((5,)), dma((3,)), dma((3,)), dma, dma,
            dma((8,)), dma((8,)), dma((4,)), dma((4,)), dma((4,)), dma((4,)),
        ],
        compiler_params=pltpu.CompilerParams(
            collective_id=1, has_side_effects=True, vmem_limit_bytes=56 * 1024 * 1024
        ),
        cost_estimate=pl.CostEstimate(flops=10_000_000_000, bytes_accessed=30_000_000, transcendentals=0),
        name="project",
    )(of, os, w_out, w_got)


def body(n, groups, queries, keys, values, frame_of_block, pair_mask, w_out):
    heads_here = queries.shape[1] // HD
    fits = n == 8 and groups == 4 and 2 * heads_here == 3 * n and queries.shape[0] == 2 * BLK
    if fits:
        return body_spread(n, queries, keys, values, frame_of_block, pair_mask, w_out)
    return body_gather(queries, keys, values, frame_of_block, pair_mask, w_out)


def solution(mesh):
    placed = (
        P("seq", "head"),
        P("seq", "head"),
        P("seq", "head"),
        P("seq"),
        P("seq", None),
        P("head", "seq"),
    )
    return jax.shard_map(
        functools.partial(body, mesh.shape["seq"], mesh.shape["head"]), mesh=mesh, in_specs=placed, out_specs=P("seq", "head"), check_vma=False
    )
```

```python
import functools
import math

import jax
import jax.numpy as jnp
from jax import lax
from jax.experimental import pallas as pl
from jax.experimental.pallas import tpu as pltpu
from jax.sharding import PartitionSpec as P

HD = 128
BLK = 256
NEG = -1e30


def body_gather(queries, keys, values, frame_of_block, pair_mask, w_out):
    tok = queries.shape[0]
    heads_here = queries.shape[1] // HD
    count_blocks = pair_mask.shape[1]
    scale = 1.0 / math.sqrt(HD)
    key_span = 512
    q_heads = queries.reshape(tok, heads_here, HD)
    q_frame = jnp.repeat(frame_of_block, BLK)
    mask_rows = jnp.repeat(pair_mask.astype(jnp.float32), BLK, axis=0)
    block_ids = jnp.arange(count_blocks, dtype=jnp.int32)

    def update(state, k_rows, v_rows, allowed):
        peak, total, accum = state
        k_heads = k_rows.reshape(k_rows.shape[0], heads_here, HD)
        v_heads = v_rows.reshape(v_rows.shape[0], heads_here, HD)
        score = (
            jnp.einsum("qhd,khd->hqk", q_heads, k_heads, preferred_element_type=jnp.float32) * scale
        )
        score = jnp.where(allowed[None], score, -1e30)
        new_peak = jnp.maximum(peak, jnp.max(score, axis=2))
        weight = jnp.where(allowed[None], jnp.exp(score - new_peak[:, :, None]), 0.0)
        factor = jnp.exp(peak - new_peak)
        new_total = total * factor + jnp.sum(weight, axis=2)
        added = jnp.einsum(
            "hqk,khd->qhd", weight.astype(jnp.bfloat16), v_heads, preferred_element_type=jnp.float32
        )
        new_accum = accum * factor.T[:, :, None] + added
        return (new_peak, new_total, new_accum)

    def attend_block(state, k_rows, v_rows, k_frame, start):
        count = k_rows.shape[0]
        k_block = (start + jnp.arange(count, dtype=jnp.int32)) // BLK
        one_hot = (block_ids[:, None] == k_block[None, :]).astype(jnp.float32)
        link = jnp.dot(mask_rows, one_hot, preferred_element_type=jnp.float32)
        same = k_frame[None, :] == q_frame[:, None]
        allowed = (k_frame[None, :] <= q_frame[:, None]) & ((link > 0.5) | same)
        return update(state, k_rows, v_rows, allowed)

    initial = (
        jnp.full((heads_here, tok), -1e30, jnp.float32),
        jnp.zeros((heads_here, tok), jnp.float32),
        jnp.zeros((tok, heads_here, HD), jnp.float32),
    )
    k_frame_local = jnp.repeat(frame_of_block, BLK)
    k_rows = lax.all_gather(keys, "seq", axis=0, tiled=True)
    v_rows = lax.all_gather(values, "seq", axis=0, tiled=True)
    k_frame = lax.all_gather(k_frame_local, "seq", axis=0, tiled=True)
    count = k_rows.shape[0]

    def step(index, inner):
        offset = (index * key_span).astype(jnp.int32)
        return attend_block(
            inner,
            lax.dynamic_slice_in_dim(k_rows, offset, key_span, 0),
            lax.dynamic_slice_in_dim(v_rows, offset, key_span, 0),
            lax.dynamic_slice_in_dim(k_frame, offset, key_span, 0),
            offset,
        )

    state = lax.fori_loop(0, count // key_span, step, initial)
    peak, total, accum = state
    attn = (accum / total.T[:, :, None]).reshape(tok, heads_here * HD).astype(jnp.bfloat16)
    terms = jnp.dot(
        attn, lax.all_gather(w_out, "seq", axis=1, tiled=True), preferred_element_type=jnp.float32
    )
    return lax.psum_scatter(terms.astype(jnp.bfloat16), "head", scatter_dimension=1, tiled=True)


def greet(n, me):
    barrier = pltpu.get_barrier_semaphore()
    for k in range(1, n):
        pl.semaphore_signal(barrier, inc=1, device_id={"seq": lax.rem(me + k, n)}, device_id_type=pl.DeviceIdType.MESH)
    pl.semaphore_wait(barrier, n - 1)


def cols(head):
    return pl.ds(pl.multiple_of(head * HD, HD), HD)


def rows(start, size):
    return pl.ds(pl.multiple_of(start, size), size)


def spread_kernel(n, tok, q, k, v, meta, qf, qs, kf, ks, vf, vs, metas, hold, hold_half, hold_meta, send, recv, here):
    me = lax.axis_index("seq")
    half = tok // 2

    def pieces(to):
        pair, odd = to // 2, lax.rem(to, 2)
        own, shared = cols(3 * pair + 2 * odd), cols(3 * pair + 1)
        full = rows(me * tok, tok)
        return [
            (meta, metas.at[rows(me * 8, 8)]),
            (q.at[:, own], qf.at[full]),
            (k.at[:, own], kf.at[full]),
            (v.at[:, own], vf.at[full]),
            (q.at[rows(odd * half, half), shared], qs.at[rows(me * half, half)]),
            (k.at[:, shared], ks.at[full]),
            (v.at[:, shared], vs.at[full]),
        ]

    def bounce(index):
        if index == 0:
            return hold_meta
        if index == 4:
            return hold_half
        return hold.at[{1: 0, 2: 1, 3: 2, 5: 3, 6: 4}[index]]

    greet(n, me)
    copies = []
    for step in range(1, n):
        to = lax.rem(me + step, n)
        for i, (src, dst) in enumerate(pieces(to)):
            copy = pltpu.make_async_remote_copy(
                src_ref=src, dst_ref=dst, send_sem=send.at[step - 1, i], recv_sem=recv.at[step - 1, i],
                device_id={"seq": to}, device_id_type=pl.DeviceIdType.MESH,
            )
            copy.start()
            copies.append(copy)
    mine = pieces(me)
    ins = [pltpu.make_async_copy(src, bounce(i), here.at[0, i]) for i, (src, _) in enumerate(mine)]
    outs = [pltpu.make_async_copy(bounce(i), dst, here.at[1, i]) for i, (_, dst) in enumerate(mine)]
    for c in ins:
        c.start()
    for c, d in zip(ins, outs):
        c.wait()
        d.start()
    for d in outs:
        d.wait()
    for c in copies:
        c.wait()


def project_kernel(
    n, tok, groups, of, os, w, wgot, out, attn, wown, wpart, part, d_send, d_recv, y_send, y_recv, final,
    send1, recv1, here, send2, recv2, wsem_s, wsem_r, dsem_s, dsem_r, ysem_s, ysem_r, osem_s, osem_r, osem_l,
):
    me, head = lax.axis_index("seq"), lax.axis_index("head")
    half = tok // 2
    wide = w.shape[1]
    early = wgot.shape[1]
    c, y = lax.rem(head, 2), head // 2
    x, zl, mine = lax.rem(me, 2), lax.rem(me // 2, 2), me // 4
    core_peer = 2 * y + 1 - c
    y_peer = 2 * (1 - y) + c

    def flip(bit, value):
        return 1 - value if bit else value

    def at(k):
        return 4 * flip(k & 4, mine) + 2 * flip(k & 2, zl) + flip(k & 1, x)

    def remote(src, dst, send, recv, seq, hd):
        return pltpu.make_async_remote_copy(
            src_ref=src, dst_ref=dst, send_sem=send, recv_sem=recv,
            device_id={"seq": seq, "head": hd}, device_id_type=pl.DeviceIdType.MESH,
        )

    barrier = pltpu.get_barrier_semaphore()
    friends = [(at(k), head) for k in range(1, n)]
    friends += [(at(k), core_peer) for k in range(4)] + [(me, y_peer)]
    for seq, hd in friends:
        pl.semaphore_signal(barrier, inc=1, device_id={"seq": seq, "head": hd}, device_id_type=pl.DeviceIdType.MESH)
    own_w = pltpu.make_async_copy(w, wown, here.at[2])
    own_w.start()
    got_w = pltpu.make_async_copy(wgot, wpart.at[:, pl.ds(0, early)], here.at[3])
    got_w.start()
    pl.semaphore_wait(barrier, len(friends))

    pair, odd = me // 2, lax.rem(me, 2)
    own, shared = cols(3 * pair + 2 * odd), cols(3 * pair + 1)

    def pieces(to):
        return [
            (of.at[rows(to * tok, tok)], attn.at[0, :, own]),
            (os.at[rows(to * half, half)], attn.at[0, rows(odd * half, half), shared]),
        ]

    back = [
        [remote(src, dst, send1.at[k, i], recv1.at[k, i], at(k), head) for i, (src, dst) in enumerate(pieces(at(k)))]
        for k in range(1, n)
    ]
    for copies in back:
        for copy in copies:
            copy.start()
    local = [pltpu.make_async_copy(src, dst, here.at[i]) for i, (src, dst) in enumerate(pieces(me))]
    for copy in local:
        copy.start()

    def chunk(at_pair):
        return pl.ds(pl.multiple_of(3 * HD * at_pair, HD), 3 * HD)

    def moves(i):
        mine_cols = chunk(at(2 * i) // 2)
        peer_cols = chunk(at((2 * i) ^ 2) // 2)
        return (
            remote(attn.at[0, :, mine_cols], attn.at[1, :, mine_cols], send2.at[0, i], recv2.at[0, i], at(1), head),
            remote(attn.at[0, :, mine_cols], attn.at[2, :, mine_cols], send2.at[1, i], recv2.at[1, i], at(2), head),
            remote(attn.at[2, :, peer_cols], attn.at[3, :, peer_cols], send2.at[2, i], recv2.at[2, i], at(1), head),
        )

    steps = [moves(i) for i in range(4)]

    def share(i):
        if i == 0:
            for copy in local:
                copy.wait()
        for k in (2 * i, 2 * i + 1):
            if k:
                for copy in back[k - 1]:
                    copy.wait_recv()
        steps[i][1].start()
        steps[i][0].start()

    def forward(i):
        steps[i][1].wait_recv()
        steps[i][2].start()

    late = [g for g, (role, first, size) in enumerate(groups) if role and first >= early]

    def w_late(g):
        _, first, size = groups[g]
        return remote(
            w.at[:, pl.ds(first, size)], wpart.at[:, pl.ds(first, size)], wsem_s.at[g], wsem_r.at[g], at(4), head
        )

    def block_of(g):
        return 1 - mine if groups[g][0] else mine

    def span(g):
        role, first, size = groups[g]
        return pl.ds(role * wide + first, size)

    def inner(g):
        return pl.ds(groups[g][1], groups[g][2])

    def swap(g, r):
        return remote(
            d_send.at[r, :, span(g)], d_recv.at[r, :, span(g)], dsem_s.at[g, r], dsem_r.at[g, r], me, core_peer
        )

    def over_y(g, r):
        return remote(
            y_send.at[r, :, inner(g)], y_recv.at[r, :, inner(g)], ysem_s.at[g, r], ysem_r.at[g, r], me, y_peer
        )

    def target(g):
        return out.at[rows(c * half, half), pl.ds(pl.multiple_of(x * wide + groups[g][1], HD), groups[g][2])]

    def home(g, r):
        return remote(
            final.at[r, :, inner(g)], target(g), osem_s.at[g, r], osem_r.at[2 * x + c, g], at(r), 2 * y + zl
        )

    def home_here(g):
        return pltpu.make_async_copy(final.at[0, :, inner(g)], target(g), osem_l.at[g])

    def multiply(g, r):
        role, first, size = groups[g]
        weights = wpart if role else wown

        def one(t, carry):
            side = (1 - c) * (1 - t) + c * t
            value = jnp.dot(
                attn[r, rows(side * half, half), :], weights[:, pl.ds(first, size)], preferred_element_type=jnp.float32
            )

            @pl.when(t == 0)
            def _():
                d_send[r, :, span(g)] = value.astype(jnp.bfloat16)
                swap(g, r).start()

            @pl.when(t == 1)
            def _():
                part[r, :, span(g)] = value

            return carry

        lax.fori_loop(0, 2, one, 0)

    def add_core(g, r):
        swap(g, r).wait_recv()

        @pl.when(y == block_of(g))
        def _():
            part[r, :, span(g)] = part[r, :, span(g)] + d_recv[r, :, span(g)].astype(jnp.float32)

        @pl.when(y != block_of(g))
        def _():
            value = part[r, :, span(g)] + d_recv[r, :, span(g)].astype(jnp.float32)
            y_send[r, :, inner(g)] = value.astype(jnp.bfloat16)
            over_y(g, r).start()

    def finish(g, r):
        @pl.when(y == block_of(g))
        def _():
            over_y(g, r).wait_recv()
            value = part[r, :, span(g)] + y_recv[r, :, inner(g)].astype(jnp.float32)
            final[r, :, inner(g)] = value.astype(jnp.bfloat16)
            if r:
                home(g, r).start()
            else:
                @pl.when(zl != c)
                def _():
                    home(g, 0).start()

                @pl.when(zl == c)
                def _():
                    home_here(g).start()

    ready = [g for g in range(len(groups)) if g not in late]

    def shard(r):
        for i, g in enumerate(ready):
            multiply(g, r)
            if i:
                add_core(ready[i - 1], r)
        add_core(ready[-1], r)

    share(0)
    share(1)
    forward(0)
    share(2)
    forward(1)
    share(3)
    for g in late:
        w_late(g).start()
    forward(2)
    own_w.wait()
    got_w.wait()
    shard(0)
    forward(3)
    for r in range(1, 4):
        for i in range(4):
            steps[i][(None, 0, 1, 2)[r]].wait_recv() if r != 2 else None
        shard(r)
        for g in ready:
            finish(g, r - 1)
    for g in ready:
        finish(g, 3)
    units = [(g, r) for g in late for r in range(4)]
    for i, (g, r) in enumerate(units):
        if r == 0:
            w_late(g).wait_recv()
        multiply(g, r)
        if i >= 1:
            add_core(*units[i - 1])
        if i >= 4:
            finish(*units[i - 4])
    add_core(*units[-1])
    for unit in units[-4:]:
        finish(*unit)

    for copies in back:
        for copy in copies:
            copy.wait_send()
    for copies in steps:
        for copy in copies:
            copy.wait_send()
    for g in late:
        w_late(g).wait_send()
    for g in range(len(groups)):
        for r in range(4):
            swap(g, r).wait_send()

            @pl.when(y != block_of(g))
            def _():
                over_y(g, r).wait_send()

            if r:
                @pl.when(y == block_of(g))
                def _():
                    home(g, r).wait_send()

        @pl.when((y == block_of(g)) & (zl != c))
        def _():
            home(g, 0).wait_send()

        @pl.when((y == block_of(g)) & (zl == c))
        def _():
            home_here(g).wait()

        for sx in range(2):
            for sc in range(2):
                piece = final.at[0, :, inner(g)]
                arrived = remote(piece, piece, osem_s.at[g, 0], osem_r.at[2 * sx + sc, g], me, core_peer)

                @pl.when((y == block_of(g)) & ((zl != c) | (sx != x) | (sc != c)))
                def _():
                    arrived.wait_recv()


def attend_kernel(odd_ref, count_ref, list_ref, qf, qs, kf, ks, vf, vs, of, os):
    odd = odd_ref[0]
    j = pl.program_id(0)
    factor = math.log2(math.e) / math.sqrt(HD)

    def scores(q, k):
        return lax.dot_general(q, k, (((1,), (1,)), ((), ())), preferred_element_type=jnp.float32)

    def fold(state, parts, vals):
        peak, total, accum = state
        top = parts[0]
        for s in parts[1:]:
            top = jnp.maximum(top, s)
        new_peak = jnp.maximum(peak, jnp.max(top, axis=1, keepdims=True))
        keep = jnp.exp2((peak - new_peak) * factor)
        total, accum = total * keep, accum * keep
        for s, v in zip(parts, vals):
            p = jnp.exp2((s - new_peak) * factor)
            for c in range(0, BLK, HD):
                total = total + p[:, c:c + HD]
            accum = accum + jnp.dot(p.astype(jnp.bfloat16), v, preferred_element_type=jnp.float32)
        return new_peak, total, accum

    def start():
        return (
            jnp.full((BLK, 1), NEG, jnp.float32),
            jnp.zeros((BLK, HD), jnp.float32),
            jnp.zeros((BLK, HD), jnp.float32),
        )

    def finish(state):
        _, total, accum = state
        return (accum / jnp.sum(total, axis=1, keepdims=True)).astype(jnp.bfloat16)

    def walk(block, streams):
        count = count_ref[block]

        def step(i, states):
            a = rows(list_ref[block, 2 * i] * BLK, BLK)
            b = rows(list_ref[block, 2 * i + 1] * BLK, BLK)
            bias = jnp.where(2 * i + 1 < count, 0.0, NEG).astype(jnp.float32)
            parts = [[scores(q, k[a, :]), scores(q, k[b, :]) + bias] for q, k, _ in streams]
            return tuple(
                fold(state, part, (v[a, :], v[b, :])) for state, part, (_, _, v) in zip(states, parts, streams)
            )

        return lax.fori_loop(0, (count + 1) // 2, step, tuple(start() for _ in streams))

    same, other = rows(odd * BLK, BLK), rows((1 - odd) * BLK, BLK)
    first, second = walk(2 * j + odd, [(qf[same, :], kf, vf), (qs[...], ks, vs)])
    of[same, :] = finish(first)
    os[...] = finish(second)
    (third,) = walk(2 * j + 1 - odd, [(qf[other, :], kf, vf)])
    of[other, :] = finish(third)


def body_spread(n, queries, keys, values, frame_of_block, pair_mask, w_out):
    tok, width = queries.shape
    count_blocks = pair_mask.shape[1]
    tokens = n * tok
    per = tok // BLK
    meta = jnp.concatenate([frame_of_block[:, None], pair_mask], axis=1)
    meta = jnp.pad(meta, ((0, 8 - per), (0, HD - 1 - count_blocks)))
    anyspace = pl.BlockSpec(memory_space=pl.ANY)
    big = jax.ShapeDtypeStruct((tokens, HD), queries.dtype)
    small = jax.ShapeDtypeStruct((tokens // 2, HD), queries.dtype)
    qf, qs, kf, ks, vf, vs, metas = pl.pallas_call(
        functools.partial(spread_kernel, n, tok),
        out_shape=[big, small, big, big, big, big, jax.ShapeDtypeStruct((8 * n, HD), jnp.int32)],
        in_specs=[anyspace] * 4,
        out_specs=[anyspace] * 7,
        scratch_shapes=[
            pltpu.VMEM((5, tok, HD), queries.dtype),
            pltpu.VMEM((tok // 2, HD), queries.dtype),
            pltpu.VMEM((8, HD), jnp.int32),
            pltpu.SemaphoreType.DMA((n - 1, 7)),
            pltpu.SemaphoreType.DMA((n - 1, 7)),
            pltpu.SemaphoreType.DMA((2, 7)),
        ],
        compiler_params=pltpu.CompilerParams(collective_id=0, has_side_effects=True),
        cost_estimate=pl.CostEstimate(flops=0, bytes_accessed=300_000_000, transcendentals=0),
        name="spread",
    )(queries, keys, values, meta)

    metas = metas.reshape(n, 8, HD)[:, :per].reshape(n * per, HD)
    frame, links = metas[:, 0], metas[:, 1:1 + count_blocks]
    allowed = (frame[None, :] <= frame[:, None]) & ((links == 1) | (frame[None, :] == frame[:, None]))
    place = jnp.cumsum(allowed.astype(jnp.int32), axis=1)
    count = place[:, -1]
    ids = jnp.arange(count_blocks, dtype=jnp.int32)
    hit = allowed[:, None, :] & (place[:, None, :] == ids[None, :, None] + 1)
    order = jnp.sum(jnp.where(hit, ids[None, None, :], 0), axis=2)
    odd = lax.rem(lax.axis_index("seq"), 2).reshape(1).astype(jnp.int32)

    smem = pl.BlockSpec(memory_space=pltpu.SMEM)
    whole = pl.BlockSpec((tokens, HD), lambda j: (0, 0))
    two = pl.BlockSpec((2 * BLK, HD), lambda j: (j, 0))
    one = pl.BlockSpec((BLK, HD), lambda j: (j, 0))
    of, os = pl.pallas_call(
        attend_kernel,
        grid=(tokens // (2 * BLK),),
        out_shape=[big, small],
        in_specs=[smem, smem, smem, two, one, whole, whole, whole, whole],
        out_specs=[two, one],
        compiler_params=pltpu.CompilerParams(vmem_limit_bytes=60 * 1024 * 1024),
        cost_estimate=pl.CostEstimate(flops=20_000_000_000, bytes_accessed=8_000_000, transcendentals=20_000_000),
        name="attend",
    )(odd, count, order, qf, qs, kf, ks, vf, vs)

    deep, wide = w_out.shape
    early = wide // 2
    w_early, _ = lax.optimization_barrier((w_out[:, :early], kf))
    w_got = lax.ppermute(w_early, "seq", [(i, (i + n // 2) % n) for i in range(n)])
    groups = [(0, 0, early), (0, early, wide - early), (1, 0, early)]
    groups += [(1, first, HD) for first in range(early, wide, HD)]
    count = len(groups)
    dma = pltpu.SemaphoreType.DMA
    return pl.pallas_call(
        functools.partial(project_kernel, n, tok, groups),
        out_shape=jax.ShapeDtypeStruct((tok, 2 * wide), queries.dtype),
        in_specs=[anyspace] * 4,
        out_specs=anyspace,
        scratch_shapes=[
            pltpu.VMEM((4, tok, width), queries.dtype),
            pltpu.VMEM((deep, wide), queries.dtype),
            pltpu.VMEM((deep, wide), queries.dtype),
            pltpu.VMEM((4, tok // 2, 2 * wide), jnp.float32),
            pltpu.VMEM((4, tok // 2, 2 * wide), queries.dtype),
            pltpu.VMEM((4, tok // 2, 2 * wide), queries.dtype),
            pltpu.VMEM((4, tok // 2, wide), queries.dtype),
            pltpu.VMEM((4, tok // 2, wide), queries.dtype),
            pltpu.VMEM((4, tok // 2, wide), queries.dtype),
            dma((n, 2)), dma((n, 2)), dma((4,)), dma((3, 4)), dma((3, 4)), dma((count,)), dma((count,)),
            dma((count, 4)), dma((count, 4)), dma((count, 4)), dma((count, 4)),
            dma((count, 4)), dma((4, count)), dma((count,)),
        ],
        compiler_params=pltpu.CompilerParams(
            collective_id=1, has_side_effects=True, vmem_limit_bytes=58 * 1024 * 1024
        ),
        cost_estimate=pl.CostEstimate(flops=10_000_000_000, bytes_accessed=30_000_000, transcendentals=0),
        name="project",
    )(of, os, w_out, w_got)


def body(n, groups, queries, keys, values, frame_of_block, pair_mask, w_out):
    heads_here = queries.shape[1] // HD
    fits = n == 8 and groups == 4 and 2 * heads_here == 3 * n and queries.shape[0] == 2 * BLK
    if fits:
        return body_spread(n, queries, keys, values, frame_of_block, pair_mask, w_out)
    return body_gather(queries, keys, values, frame_of_block, pair_mask, w_out)


def solution(mesh):
    placed = (
        P("seq", "head"),
        P("seq", "head"),
        P("seq", "head"),
        P("seq"),
        P("seq", None),
        P("head", "seq"),
    )
    return jax.shard_map(
        functools.partial(body, mesh.shape["seq"], mesh.shape["head"]), mesh=mesh, in_specs=placed, out_specs=P("seq", "head"), check_vma=False
    )
```

```python
import functools
import math

import jax
import jax.numpy as jnp
from jax import lax
from jax.experimental import pallas as pl
from jax.experimental.pallas import tpu as pltpu
from jax.sharding import PartitionSpec as P

HD = 128
BLK = 256
NEG = -1e30


def body_gather(queries, keys, values, frame_of_block, pair_mask, w_out):
    tok = queries.shape[0]
    heads_here = queries.shape[1] // HD
    count_blocks = pair_mask.shape[1]
    scale = 1.0 / math.sqrt(HD)
    key_span = 512
    q_heads = queries.reshape(tok, heads_here, HD)
    q_frame = jnp.repeat(frame_of_block, BLK)
    mask_rows = jnp.repeat(pair_mask.astype(jnp.float32), BLK, axis=0)
    block_ids = jnp.arange(count_blocks, dtype=jnp.int32)

    def update(state, k_rows, v_rows, allowed):
        peak, total, accum = state
        k_heads = k_rows.reshape(k_rows.shape[0], heads_here, HD)
        v_heads = v_rows.reshape(v_rows.shape[0], heads_here, HD)
        score = (
            jnp.einsum("qhd,khd->hqk", q_heads, k_heads, preferred_element_type=jnp.float32) * scale
        )
        score = jnp.where(allowed[None], score, -1e30)
        new_peak = jnp.maximum(peak, jnp.max(score, axis=2))
        weight = jnp.where(allowed[None], jnp.exp(score - new_peak[:, :, None]), 0.0)
        factor = jnp.exp(peak - new_peak)
        new_total = total * factor + jnp.sum(weight, axis=2)
        added = jnp.einsum(
            "hqk,khd->qhd", weight.astype(jnp.bfloat16), v_heads, preferred_element_type=jnp.float32
        )
        new_accum = accum * factor.T[:, :, None] + added
        return (new_peak, new_total, new_accum)

    def attend_block(state, k_rows, v_rows, k_frame, start):
        count = k_rows.shape[0]
        k_block = (start + jnp.arange(count, dtype=jnp.int32)) // BLK
        one_hot = (block_ids[:, None] == k_block[None, :]).astype(jnp.float32)
        link = jnp.dot(mask_rows, one_hot, preferred_element_type=jnp.float32)
        same = k_frame[None, :] == q_frame[:, None]
        allowed = (k_frame[None, :] <= q_frame[:, None]) & ((link > 0.5) | same)
        return update(state, k_rows, v_rows, allowed)

    initial = (
        jnp.full((heads_here, tok), -1e30, jnp.float32),
        jnp.zeros((heads_here, tok), jnp.float32),
        jnp.zeros((tok, heads_here, HD), jnp.float32),
    )
    k_frame_local = jnp.repeat(frame_of_block, BLK)
    k_rows = lax.all_gather(keys, "seq", axis=0, tiled=True)
    v_rows = lax.all_gather(values, "seq", axis=0, tiled=True)
    k_frame = lax.all_gather(k_frame_local, "seq", axis=0, tiled=True)
    count = k_rows.shape[0]

    def step(index, inner):
        offset = (index * key_span).astype(jnp.int32)
        return attend_block(
            inner,
            lax.dynamic_slice_in_dim(k_rows, offset, key_span, 0),
            lax.dynamic_slice_in_dim(v_rows, offset, key_span, 0),
            lax.dynamic_slice_in_dim(k_frame, offset, key_span, 0),
            offset,
        )

    state = lax.fori_loop(0, count // key_span, step, initial)
    peak, total, accum = state
    attn = (accum / total.T[:, :, None]).reshape(tok, heads_here * HD).astype(jnp.bfloat16)
    terms = jnp.dot(
        attn, lax.all_gather(w_out, "seq", axis=1, tiled=True), preferred_element_type=jnp.float32
    )
    return lax.psum_scatter(terms.astype(jnp.bfloat16), "head", scatter_dimension=1, tiled=True)


def flip(bit, value):
    return 1 - value if bit else value


def greet(plane):
    barrier = pltpu.get_barrier_semaphore()
    for seq, head in plane:
        pl.semaphore_signal(
            barrier, inc=1, device_id={"seq": seq, "head": head}, device_id_type=pl.DeviceIdType.MESH
        )
    return lambda: pl.semaphore_wait(barrier, len(plane))


def remote(src, dst, send, recv, seq, head):
    return pltpu.make_async_remote_copy(
        src_ref=src, dst_ref=dst, send_sem=send, recv_sem=recv,
        device_id={"seq": seq, "head": head}, device_id_type=pl.DeviceIdType.MESH,
    )


def cols(head):
    return pl.ds(pl.multiple_of(head * HD, HD), HD)


def rows(start, size):
    return pl.ds(pl.multiple_of(start, size), size)


def spread_kernel(
    n, tok, q, k, v, meta, qf, qs, kf, ks, vf, vs, metas,
    hold, hold_half, hold_meta, send, recv, here, fsem_s, fsem_r,
):
    me, head = lax.axis_index("seq"), lax.axis_index("head")
    half = tok // 2
    x, zl, zh = lax.rem(me, 2), lax.rem(me // 2, 2), me // 4
    c, y = lax.rem(head, 2), head // 2
    other = 2 * y + 1 - c
    cross = x * (1 - c) + (1 - x) * c

    def layer(i):
        return 2 * flip(i & 2, zh) + flip(i & 1, zl)

    def pieces(i, far):
        pair, core = layer(i), flip(far, c)
        own, shared = cols(3 * pair + 2 * core), cols(3 * pair + 1)
        full = rows(me * tok, tok)
        return [
            (q.at[:, own], qf.at[full]),
            (k.at[:, own], kf.at[full]),
            (v.at[:, own], vf.at[full]),
            (q.at[rows(core * half, half), shared], qs.at[rows(me * half, half)]),
            (v.at[:, shared], vs.at[full]) if far else (k.at[:, shared], ks.at[full]),
            (meta, metas.at[rows(me * 8, 8)]),
        ]

    def out_copies(i, far):
        return [
            remote(src, dst, send.at[i, far, p], recv.at[i, cross, p], 2 * layer(i) + c, 2 * y + flip(far, c))
            for p, (src, dst) in enumerate(pieces(i, far))
        ]

    def from_row(i, side):
        return 2 * layer(i) + flip(side, x)

    def forward(i, side, keys):
        piece = (ks if keys else vs).at[rows(from_row(i, side) * tok, tok)]
        return remote(piece, piece, fsem_s.at[i, side], fsem_r.at[i, side], me, other)

    greet([(2 * layer(i) + flip(side, x), 2 * y + core) for i in range(4) for side in range(2) for core in range(2)
           if i or side] + [(me, other)])()
    for i in (2, 3, 1):
        for far in range(2):
            for copy in out_copies(i, far):
                copy.start()
    for copy in out_copies(0, 1):
        copy.start()

    @pl.when(x != c)
    def _():
        for copy in out_copies(0, 0):
            copy.start()

    @pl.when(x == c)
    def _():
        mine = pieces(0, 0)
        via = [hold.at[0], hold.at[1], hold.at[2], hold_half, hold.at[3], hold_meta]
        ins = [pltpu.make_async_copy(src, mid, here.at[0, p]) for p, ((src, _), mid) in enumerate(zip(mine, via))]
        outs = [pltpu.make_async_copy(mid, dst, here.at[1, p]) for p, ((_, dst), mid) in enumerate(zip(mine, via))]
        for one in ins:
            one.start()
        for one, two in zip(ins, outs):
            one.wait()
            two.start()
        for two in outs:
            two.wait()

    def arrive(i, side):
        for p, (_, dst) in enumerate(pieces(i, 0)):
            remote(dst, dst, send.at[i, 0, p], recv.at[i, side, p], me, other).wait_recv()

    for i in (0, 1, 2, 3):
        for side in range(2):
            if i or side:
                arrive(i, side)
            else:
                @pl.when(x != c)
                def _():
                    arrive(0, 0)

            for keys in (True, False):
                @pl.when((x == c) == keys)
                def _():
                    forward(i, side, keys).start()

    for i in range(4):
        for side in range(2):
            for keys in (True, False):
                @pl.when((x == c) == keys)
                def _():
                    forward(i, side, keys).wait_send()
                    forward(i, side, not keys).wait_recv()

        for far in range(2):
            if i or far:
                for copy in out_copies(i, far):
                    copy.wait_send()
            else:
                @pl.when(x != c)
                def _():
                    for copy in out_copies(0, 0):
                        copy.wait_send()


def project_kernel(
    n, tok, groups, of, os, w, wgot, out, attn, wown, wpart, part, d_send, d_recv, y_send, y_recv, final,
    send1, recv1, here, send2, recv2, wsem_s, wsem_r, dsem_s, dsem_r, ysem_s, ysem_r, osem_s, osem_r, osem_l,
):
    me, head = lax.axis_index("seq"), lax.axis_index("head")
    half = tok // 2
    wide = w.shape[1]
    early = wgot.shape[1]
    c, y = lax.rem(head, 2), head // 2
    x, zl, mine = lax.rem(me, 2), lax.rem(me // 2, 2), me // 4
    core_peer = 2 * y + 1 - c
    y_peer = 2 * (1 - y) + c

    def at(k):
        return 4 * flip(k & 4, mine) + 2 * flip(k & 2, zl) + flip(k & 1, x)

    met = greet([(at(k), 2 * y + core) for k in range(1, n) for core in range(2)] + [(me, core_peer), (me, y_peer)])
    own_w = pltpu.make_async_copy(w, wown, here.at[2])
    own_w.start()
    got_w = pltpu.make_async_copy(wgot, wpart.at[:, pl.ds(0, early)], here.at[3])
    got_w.start()
    met()

    own, shared = cols(3 * (me // 2) + 2 * c), cols(3 * (me // 2) + 1)

    def pieces(to):
        return [
            (of.at[rows(to * tok, tok)], attn.at[0, :, own]),
            (os.at[rows(to * half, half)], attn.at[0, rows(c * half, half), shared]),
        ]

    def back(k):
        return [
            remote(src, dst, send1.at[k, p], recv1.at[k // 2, c, p], at(k), 2 * y + x)
            for p, (src, dst) in enumerate(pieces(at(k)))
        ]

    local = [pltpu.make_async_copy(src, dst, here.at[p]) for p, (src, dst) in enumerate(pieces(me))]
    for k in range(1, n):
        for copy in back(k):
            copy.start()

    @pl.when(c != x)
    def _():
        for copy in back(0):
            copy.start()

    @pl.when(c == x)
    def _():
        for copy in local:
            copy.start()

    def chunk(at_pair):
        return pl.ds(pl.multiple_of(3 * HD * at_pair, HD), 3 * HD)

    def moves(i):
        mine_cols = chunk(at(2 * i) // 2)
        peer_cols = chunk(at((2 * i) ^ 2) // 2)
        return (
            remote(attn.at[0, :, mine_cols], attn.at[1, :, mine_cols], send2.at[0, i], recv2.at[0, i], at(1), head),
            remote(attn.at[0, :, mine_cols], attn.at[2, :, mine_cols], send2.at[1, i], recv2.at[1, i], at(2), head),
            remote(attn.at[2, :, peer_cols], attn.at[3, :, peer_cols], send2.at[2, i], recv2.at[2, i], at(1), head),
        )

    steps = [moves(i) for i in range(4)]

    def share(i):
        for core in range(2):
            for p, (_, dst) in enumerate(pieces(me)):
                arrived = remote(dst, dst, send1.at[0, p], recv1.at[i, core, p], me, core_peer)
                if i:
                    arrived.wait_recv()
                else:
                    @pl.when((c != x) | (core != c))
                    def _():
                        arrived.wait_recv()

        if i == 0:
            @pl.when(c == x)
            def _():
                for copy in local:
                    copy.wait()

        steps[i][1].start()
        steps[i][0].start()

    def forward(i):
        steps[i][1].wait_recv()
        steps[i][2].start()

    late = [g for g, (role, first, size) in enumerate(groups) if role and first >= early]

    def w_late(g):
        _, first, size = groups[g]
        return remote(
            w.at[:, pl.ds(first, size)], wpart.at[:, pl.ds(first, size)], wsem_s.at[g], wsem_r.at[g], at(4), head
        )

    def block_of(g):
        return 1 - mine if groups[g][0] else mine

    def span(g):
        role, first, size = groups[g]
        return pl.ds(role * wide + first, size)

    def inner(g):
        return pl.ds(groups[g][1], groups[g][2])

    def swap(g, r):
        return remote(
            d_send.at[r, :, span(g)], d_recv.at[r, :, span(g)], dsem_s.at[g, r], dsem_r.at[g, r], me, core_peer
        )

    def over_y(g, r):
        return remote(
            y_send.at[r, :, inner(g)], y_recv.at[r, :, inner(g)], ysem_s.at[g, r], ysem_r.at[g, r], me, y_peer
        )

    def target(g):
        return out.at[rows(c * half, half), pl.ds(pl.multiple_of(x * wide + groups[g][1], HD), groups[g][2])]

    def home(g, r):
        return remote(
            final.at[r, :, inner(g)], target(g), osem_s.at[g, r], osem_r.at[2 * x + c, g], at(r), 2 * y + zl
        )

    def home_here(g):
        return pltpu.make_async_copy(final.at[0, :, inner(g)], target(g), osem_l.at[g])

    def multiply(g, r):
        role, first, size = groups[g]
        weights = wpart if role else wown

        def one(t, carry):
            side = (1 - c) * (1 - t) + c * t
            value = jnp.dot(
                attn[r, rows(side * half, half), :], weights[:, pl.ds(first, size)], preferred_element_type=jnp.float32
            )

            @pl.when(t == 0)
            def _():
                d_send[r, :, span(g)] = value.astype(jnp.bfloat16)
                swap(g, r).start()

            @pl.when(t == 1)
            def _():
                part[r, :, span(g)] = value

            return carry

        lax.fori_loop(0, 2, one, 0)

    def add_core(g, r):
        swap(g, r).wait_recv()

        @pl.when(y == block_of(g))
        def _():
            part[r, :, span(g)] = part[r, :, span(g)] + d_recv[r, :, span(g)].astype(jnp.float32)

        @pl.when(y != block_of(g))
        def _():
            value = part[r, :, span(g)] + d_recv[r, :, span(g)].astype(jnp.float32)
            y_send[r, :, inner(g)] = value.astype(jnp.bfloat16)
            over_y(g, r).start()

    def finish(g, r):
        @pl.when(y == block_of(g))
        def _():
            over_y(g, r).wait_recv()
            value = part[r, :, span(g)] + y_recv[r, :, inner(g)].astype(jnp.float32)
            final[r, :, inner(g)] = value.astype(jnp.bfloat16)
            if r:
                home(g, r).start()
            else:
                @pl.when(zl != c)
                def _():
                    home(g, 0).start()

                @pl.when(zl == c)
                def _():
                    home_here(g).start()

    ready = [g for g in range(len(groups)) if g not in late]

    def shard(r):
        for i, g in enumerate(ready):
            multiply(g, r)
            if i:
                add_core(ready[i - 1], r)
        add_core(ready[-1], r)

    share(0)
    share(1)
    forward(0)
    share(2)
    forward(1)
    share(3)
    for g in late:
        w_late(g).start()
    forward(2)
    own_w.wait()
    got_w.wait()
    shard(0)
    forward(3)
    for r in range(1, 4):
        for i in range(4):
            steps[i][(None, 0, 1, 2)[r]].wait_recv() if r != 2 else None
        shard(r)
        for g in ready:
            finish(g, r - 1)
    for g in ready:
        finish(g, 3)
    units = [(g, r) for g in late for r in range(4)]
    for i, (g, r) in enumerate(units):
        if r == 0:
            w_late(g).wait_recv()
        multiply(g, r)
        if i >= 1:
            add_core(*units[i - 1])
        if i >= 4:
            finish(*units[i - 4])
    add_core(*units[-1])
    for unit in units[-4:]:
        finish(*unit)

    for k in range(1, n):
        for copy in back(k):
            copy.wait_send()

    @pl.when(c != x)
    def _():
        for copy in back(0):
            copy.wait_send()

    for copies in steps:
        for copy in copies:
            copy.wait_send()
    for g in late:
        w_late(g).wait_send()
    for g in range(len(groups)):
        for r in range(4):
            swap(g, r).wait_send()

            @pl.when(y != block_of(g))
            def _():
                over_y(g, r).wait_send()

            if r:
                @pl.when(y == block_of(g))
                def _():
                    home(g, r).wait_send()

        @pl.when((y == block_of(g)) & (zl != c))
        def _():
            home(g, 0).wait_send()

        @pl.when((y == block_of(g)) & (zl == c))
        def _():
            home_here(g).wait()

        for sx in range(2):
            for sc in range(2):
                piece = final.at[0, :, inner(g)]
                arrived = remote(piece, piece, osem_s.at[g, 0], osem_r.at[2 * sx + sc, g], me, core_peer)

                @pl.when((y == block_of(g)) & ((zl != c) | (sx != x) | (sc != c)))
                def _():
                    arrived.wait_recv()


def attend_kernel(odd_ref, count_ref, list_ref, qf, qs, kf, ks, vf, vs, of, os):
    odd = odd_ref[0]
    j = pl.program_id(0)
    factor = math.log2(math.e) / math.sqrt(HD)

    def scores(q, k):
        return lax.dot_general(q, k, (((1,), (1,)), ((), ())), preferred_element_type=jnp.float32)

    def fold(state, parts, vals):
        peak, total, accum = state
        top = parts[0]
        for s in parts[1:]:
            top = jnp.maximum(top, s)
        new_peak = jnp.maximum(peak, jnp.max(top, axis=1, keepdims=True))
        keep = jnp.exp2((peak - new_peak) * factor)
        total, accum = total * keep, accum * keep
        for s, v in zip(parts, vals):
            p = jnp.exp2((s - new_peak) * factor)
            for c in range(0, BLK, HD):
                total = total + p[:, c:c + HD]
            accum = accum + jnp.dot(p.astype(jnp.bfloat16), v, preferred_element_type=jnp.float32)
        return new_peak, total, accum

    def start():
        return (
            jnp.full((BLK, 1), NEG, jnp.float32),
            jnp.zeros((BLK, HD), jnp.float32),
            jnp.zeros((BLK, HD), jnp.float32),
        )

    def finish(state):
        _, total, accum = state
        return (accum / jnp.sum(total, axis=1, keepdims=True)).astype(jnp.bfloat16)

    def walk(block, streams):
        count = count_ref[block]

        def step(i, states):
            a = rows(list_ref[block, 2 * i] * BLK, BLK)
            b = rows(list_ref[block, 2 * i + 1] * BLK, BLK)
            bias = jnp.where(2 * i + 1 < count, 0.0, NEG).astype(jnp.float32)
            parts = [[scores(q, k[a, :]), scores(q, k[b, :]) + bias] for q, k, _ in streams]
            return tuple(
                fold(state, part, (v[a, :], v[b, :])) for state, part, (_, _, v) in zip(states, parts, streams)
            )

        return lax.fori_loop(0, (count + 1) // 2, step, tuple(start() for _ in streams))

    same, other = rows(odd * BLK, BLK), rows((1 - odd) * BLK, BLK)
    first, second = walk(2 * j + odd, [(qf[same, :], kf, vf), (qs[...], ks, vs)])
    of[same, :] = finish(first)
    os[...] = finish(second)
    (third,) = walk(2 * j + 1 - odd, [(qf[other, :], kf, vf)])
    of[other, :] = finish(third)


def body_spread(n, queries, keys, values, frame_of_block, pair_mask, w_out):
    tok, width = queries.shape
    count_blocks = pair_mask.shape[1]
    tokens = n * tok
    per = tok // BLK
    meta = jnp.concatenate([frame_of_block[:, None], pair_mask], axis=1)
    meta = jnp.pad(meta, ((0, 8 - per), (0, HD - 1 - count_blocks)))
    anyspace = pl.BlockSpec(memory_space=pl.ANY)
    big = jax.ShapeDtypeStruct((tokens, HD), queries.dtype)
    small = jax.ShapeDtypeStruct((tokens // 2, HD), queries.dtype)
    qf, qs, kf, ks, vf, vs, metas = pl.pallas_call(
        functools.partial(spread_kernel, n, tok),
        out_shape=[big, small, big, big, big, big, jax.ShapeDtypeStruct((8 * n, HD), jnp.int32)],
        in_specs=[anyspace] * 4,
        out_specs=[anyspace] * 7,
        scratch_shapes=[
            pltpu.VMEM((4, tok, HD), queries.dtype),
            pltpu.VMEM((tok // 2, HD), queries.dtype),
            pltpu.VMEM((8, HD), jnp.int32),
            pltpu.SemaphoreType.DMA((4, 2, 6)),
            pltpu.SemaphoreType.DMA((4, 2, 6)),
            pltpu.SemaphoreType.DMA((2, 6)),
            pltpu.SemaphoreType.DMA((4, 2)),
            pltpu.SemaphoreType.DMA((4, 2)),
        ],
        compiler_params=pltpu.CompilerParams(collective_id=0, has_side_effects=True),
        cost_estimate=pl.CostEstimate(flops=0, bytes_accessed=300_000_000, transcendentals=0),
        name="spread",
    )(queries, keys, values, meta)

    metas = metas.reshape(n, 8, HD)[:, :per].reshape(n * per, HD)
    frame, links = metas[:, 0], metas[:, 1:1 + count_blocks]
    allowed = (frame[None, :] <= frame[:, None]) & ((links == 1) | (frame[None, :] == frame[:, None]))
    place = jnp.cumsum(allowed.astype(jnp.int32), axis=1)
    count = place[:, -1]
    ids = jnp.arange(count_blocks, dtype=jnp.int32)
    hit = allowed[:, None, :] & (place[:, None, :] == ids[None, :, None] + 1)
    order = jnp.sum(jnp.where(hit, ids[None, None, :], 0), axis=2)
    odd = lax.rem(lax.axis_index("head"), 2).reshape(1).astype(jnp.int32)

    smem = pl.BlockSpec(memory_space=pltpu.SMEM)
    whole = pl.BlockSpec((tokens, HD), lambda j: (0, 0))
    two = pl.BlockSpec((2 * BLK, HD), lambda j: (j, 0))
    one = pl.BlockSpec((BLK, HD), lambda j: (j, 0))
    of, os = pl.pallas_call(
        attend_kernel,
        grid=(tokens // (2 * BLK),),
        out_shape=[big, small],
        in_specs=[smem, smem, smem, two, one, whole, whole, whole, whole],
        out_specs=[two, one],
        compiler_params=pltpu.CompilerParams(vmem_limit_bytes=60 * 1024 * 1024),
        cost_estimate=pl.CostEstimate(flops=20_000_000_000, bytes_accessed=8_000_000, transcendentals=20_000_000),
        name="attend",
    )(odd, count, order, qf, qs, kf, ks, vf, vs)

    deep, wide = w_out.shape
    early = wide // 2
    w_early, _ = lax.optimization_barrier((w_out[:, :early], kf))
    w_got = lax.ppermute(w_early, "seq", [(i, (i + n // 2) % n) for i in range(n)])
    groups = [(0, 0, early), (0, early, wide - early), (1, 0, early)]
    groups += [(1, first, HD) for first in range(early, wide, HD)]
    count = len(groups)
    dma = pltpu.SemaphoreType.DMA
    return pl.pallas_call(
        functools.partial(project_kernel, n, tok, groups),
        out_shape=jax.ShapeDtypeStruct((tok, 2 * wide), queries.dtype),
        in_specs=[anyspace] * 4,
        out_specs=anyspace,
        scratch_shapes=[
            pltpu.VMEM((4, tok, width), queries.dtype),
            pltpu.VMEM((deep, wide), queries.dtype),
            pltpu.VMEM((deep, wide), queries.dtype),
            pltpu.VMEM((4, tok // 2, 2 * wide), jnp.float32),
            pltpu.VMEM((4, tok // 2, 2 * wide), queries.dtype),
            pltpu.VMEM((4, tok // 2, 2 * wide), queries.dtype),
            pltpu.VMEM((4, tok // 2, wide), queries.dtype),
            pltpu.VMEM((4, tok // 2, wide), queries.dtype),
            pltpu.VMEM((4, tok // 2, wide), queries.dtype),
            dma((n, 2)), dma((4, 2, 2)), dma((4,)), dma((3, 4)), dma((3, 4)), dma((count,)), dma((count,)),
            dma((count, 4)), dma((count, 4)), dma((count, 4)), dma((count, 4)),
            dma((count, 4)), dma((4, count)), dma((count,)),
        ],
        compiler_params=pltpu.CompilerParams(
            collective_id=1, has_side_effects=True, vmem_limit_bytes=58 * 1024 * 1024
        ),
        cost_estimate=pl.CostEstimate(flops=10_000_000_000, bytes_accessed=30_000_000, transcendentals=0),
        name="project",
    )(of, os, w_out, w_got)


def body(n, groups, queries, keys, values, frame_of_block, pair_mask, w_out):
    heads_here = queries.shape[1] // HD
    fits = n == 8 and groups == 4 and 2 * heads_here == 3 * n and queries.shape[0] == 2 * BLK
    if fits:
        return body_spread(n, queries, keys, values, frame_of_block, pair_mask, w_out)
    return body_gather(queries, keys, values, frame_of_block, pair_mask, w_out)


def solution(mesh):
    placed = (
        P("seq", "head"),
        P("seq", "head"),
        P("seq", "head"),
        P("seq"),
        P("seq", None),
        P("head", "seq"),
    )
    return jax.shard_map(
        functools.partial(body, mesh.shape["seq"], mesh.shape["head"]), mesh=mesh, in_specs=placed, out_specs=P("seq", "head"), check_vma=False
    )
```

```python
import functools
import math

import jax
import jax.numpy as jnp
from jax import lax
from jax.experimental import pallas as pl
from jax.experimental.pallas import tpu as pltpu
from jax.sharding import PartitionSpec as P

HD = 128
BLK = 256
NEG = -1e30


def body_gather(queries, keys, values, frame_of_block, pair_mask, w_out):
    tok = queries.shape[0]
    heads_here = queries.shape[1] // HD
    count_blocks = pair_mask.shape[1]
    scale = 1.0 / math.sqrt(HD)
    key_span = 512
    q_heads = queries.reshape(tok, heads_here, HD)
    q_frame = jnp.repeat(frame_of_block, BLK)
    mask_rows = jnp.repeat(pair_mask.astype(jnp.float32), BLK, axis=0)
    block_ids = jnp.arange(count_blocks, dtype=jnp.int32)

    def update(state, k_rows, v_rows, allowed):
        peak, total, accum = state
        k_heads = k_rows.reshape(k_rows.shape[0], heads_here, HD)
        v_heads = v_rows.reshape(v_rows.shape[0], heads_here, HD)
        score = (
            jnp.einsum("qhd,khd->hqk", q_heads, k_heads, preferred_element_type=jnp.float32) * scale
        )
        score = jnp.where(allowed[None], score, -1e30)
        new_peak = jnp.maximum(peak, jnp.max(score, axis=2))
        weight = jnp.where(allowed[None], jnp.exp(score - new_peak[:, :, None]), 0.0)
        factor = jnp.exp(peak - new_peak)
        new_total = total * factor + jnp.sum(weight, axis=2)
        added = jnp.einsum(
            "hqk,khd->qhd", weight.astype(jnp.bfloat16), v_heads, preferred_element_type=jnp.float32
        )
        new_accum = accum * factor.T[:, :, None] + added
        return (new_peak, new_total, new_accum)

    def attend_block(state, k_rows, v_rows, k_frame, start):
        count = k_rows.shape[0]
        k_block = (start + jnp.arange(count, dtype=jnp.int32)) // BLK
        one_hot = (block_ids[:, None] == k_block[None, :]).astype(jnp.float32)
        link = jnp.dot(mask_rows, one_hot, preferred_element_type=jnp.float32)
        same = k_frame[None, :] == q_frame[:, None]
        allowed = (k_frame[None, :] <= q_frame[:, None]) & ((link > 0.5) | same)
        return update(state, k_rows, v_rows, allowed)

    initial = (
        jnp.full((heads_here, tok), -1e30, jnp.float32),
        jnp.zeros((heads_here, tok), jnp.float32),
        jnp.zeros((tok, heads_here, HD), jnp.float32),
    )
    k_frame_local = jnp.repeat(frame_of_block, BLK)
    k_rows = lax.all_gather(keys, "seq", axis=0, tiled=True)
    v_rows = lax.all_gather(values, "seq", axis=0, tiled=True)
    k_frame = lax.all_gather(k_frame_local, "seq", axis=0, tiled=True)
    count = k_rows.shape[0]

    def step(index, inner):
        offset = (index * key_span).astype(jnp.int32)
        return attend_block(
            inner,
            lax.dynamic_slice_in_dim(k_rows, offset, key_span, 0),
            lax.dynamic_slice_in_dim(v_rows, offset, key_span, 0),
            lax.dynamic_slice_in_dim(k_frame, offset, key_span, 0),
            offset,
        )

    state = lax.fori_loop(0, count // key_span, step, initial)
    peak, total, accum = state
    attn = (accum / total.T[:, :, None]).reshape(tok, heads_here * HD).astype(jnp.bfloat16)
    terms = jnp.dot(
        attn, lax.all_gather(w_out, "seq", axis=1, tiled=True), preferred_element_type=jnp.float32
    )
    return lax.psum_scatter(terms.astype(jnp.bfloat16), "head", scatter_dimension=1, tiled=True)


def flip(bit, value):
    return 1 - value if bit else value


def greet(plane):
    barrier = pltpu.get_barrier_semaphore()
    for seq, head in plane:
        pl.semaphore_signal(
            barrier, inc=1, device_id={"seq": seq, "head": head}, device_id_type=pl.DeviceIdType.MESH
        )
    return lambda: pl.semaphore_wait(barrier, len(plane))


def remote(src, dst, send, recv, seq, head):
    return pltpu.make_async_remote_copy(
        src_ref=src, dst_ref=dst, send_sem=send, recv_sem=recv,
        device_id={"seq": seq, "head": head}, device_id_type=pl.DeviceIdType.MESH,
    )


def cols(head):
    return pl.ds(pl.multiple_of(head * HD, HD), HD)


def rows(start, size):
    return pl.ds(pl.multiple_of(start, size), size)


def spread_kernel(
    n, tok, q, k, v, meta, qf, qs, kf, ks, vf, vs, metas,
    hold, hold_half, hold_meta, send, recv, here, fsem_s, fsem_r,
):
    me, head = lax.axis_index("seq"), lax.axis_index("head")
    half = tok // 2
    x, zl, zh = lax.rem(me, 2), lax.rem(me // 2, 2), me // 4
    c, y = lax.rem(head, 2), head // 2
    other = 2 * y + 1 - c
    cross = x * (1 - c) + (1 - x) * c

    def layer(i):
        return 2 * flip(i & 2, zh) + flip(i & 1, zl)

    def pieces(i, far):
        pair, core = layer(i), flip(far, c)
        own, shared = cols(3 * pair + 2 * core), cols(3 * pair + 1)
        full = rows(me * tok, tok)
        return [
            (q.at[:, own], qf.at[full]),
            (k.at[:, own], kf.at[full]),
            (v.at[:, own], vf.at[full]),
            (q.at[rows(core * half, half), shared], qs.at[rows(me * half, half)]),
            (v.at[:, shared], vs.at[full]) if far else (k.at[:, shared], ks.at[full]),
            (meta, metas.at[rows(me * 8, 8)]),
        ]

    def out_copies(i, far):
        return [
            remote(src, dst, send.at[i, far, p], recv.at[i, cross, p], 2 * layer(i) + c, 2 * y + flip(far, c))
            for p, (src, dst) in enumerate(pieces(i, far))
        ]

    def from_row(i, side):
        return 2 * layer(i) + flip(side, x)

    def forward(i, side, keys):
        piece = (ks if keys else vs).at[rows(from_row(i, side) * tok, tok)]
        return remote(piece, piece, fsem_s.at[i, side], fsem_r.at[i, side], me, other)

    greet([(2 * layer(i) + flip(side, x), 2 * y + core) for i in range(4) for side in range(2) for core in range(2)
           if i or side] + [(me, other)])()
    for i in (2, 3, 1):
        for far in range(2):
            for copy in out_copies(i, far):
                copy.start()
    for copy in out_copies(0, 1):
        copy.start()

    @pl.when(x != c)
    def _():
        for copy in out_copies(0, 0):
            copy.start()

    @pl.when(x == c)
    def _():
        mine = pieces(0, 0)
        via = [hold.at[0], hold.at[1], hold.at[2], hold_half, hold.at[3], hold_meta]
        ins = [pltpu.make_async_copy(src, mid, here.at[0, p]) for p, ((src, _), mid) in enumerate(zip(mine, via))]
        outs = [pltpu.make_async_copy(mid, dst, here.at[1, p]) for p, ((_, dst), mid) in enumerate(zip(mine, via))]
        for one in ins:
            one.start()
        for one, two in zip(ins, outs):
            one.wait()
            two.start()
        for two in outs:
            two.wait()

    def arrive(i, side):
        for p, (_, dst) in enumerate(pieces(i, 0)):
            remote(dst, dst, send.at[i, 0, p], recv.at[i, side, p], me, other).wait_recv()

    for i in (0, 1, 2, 3):
        for side in range(2):
            if i or side:
                arrive(i, side)
            else:
                @pl.when(x != c)
                def _():
                    arrive(0, 0)

            for keys in (True, False):
                @pl.when((x == c) == keys)
                def _():
                    forward(i, side, keys).start()

    for i in range(4):
        for side in range(2):
            for keys in (True, False):
                @pl.when((x == c) == keys)
                def _():
                    forward(i, side, keys).wait_send()
                    forward(i, side, not keys).wait_recv()

        for far in range(2):
            if i or far:
                for copy in out_copies(i, far):
                    copy.wait_send()
            else:
                @pl.when(x != c)
                def _():
                    for copy in out_copies(0, 0):
                        copy.wait_send()


def project_kernel(
    n, tok, groups, of, os, w, wgot, out, attn, wown, wpart, part, d_send, d_recv, y_send, y_recv, final,
    send1, recv1, here, send2, recv2, wsem_s, wsem_r, dsem_s, dsem_r, ysem_s, ysem_r, osem_s, osem_r, osem_l,
):
    me, head = lax.axis_index("seq"), lax.axis_index("head")
    half = tok // 2
    wide = w.shape[1]
    early = wgot.shape[1]
    c, y = lax.rem(head, 2), head // 2
    x, zl, mine = lax.rem(me, 2), lax.rem(me // 2, 2), me // 4
    core_peer = 2 * y + 1 - c
    y_peer = 2 * (1 - y) + c

    def at(k):
        return 4 * flip(k & 4, mine) + 2 * flip(k & 2, zl) + flip(k & 1, x)

    met = greet([(at(k), 2 * y + core) for k in range(1, n) for core in range(2)] + [(me, core_peer), (me, y_peer)])
    own_w = pltpu.make_async_copy(w, wown, here.at[2])
    own_w.start()
    got_w = pltpu.make_async_copy(wgot, wpart.at[:, pl.ds(0, early)], here.at[3])
    got_w.start()
    met()

    own, shared = cols(3 * (me // 2) + 2 * c), cols(3 * (me // 2) + 1)

    def pieces(to):
        return [
            (of.at[rows(to * tok, tok)], attn.at[0, :, own]),
            (os.at[rows(to * half, half)], attn.at[0, rows(c * half, half), shared]),
        ]

    def back(k):
        return [
            remote(src, dst, send1.at[k, p], recv1.at[k // 2, c, p], at(k), 2 * y + x)
            for p, (src, dst) in enumerate(pieces(at(k)))
        ]

    local = [pltpu.make_async_copy(src, dst, here.at[p]) for p, (src, dst) in enumerate(pieces(me))]
    for k in range(1, n):
        for copy in back(k):
            copy.start()

    @pl.when(c != x)
    def _():
        for copy in back(0):
            copy.start()

    @pl.when(c == x)
    def _():
        for copy in local:
            copy.start()

    def chunk(at_pair):
        return pl.ds(pl.multiple_of(3 * HD * at_pair, HD), 3 * HD)

    def moves(i):
        mine_cols = chunk(at(2 * i) // 2)
        peer_cols = chunk(at((2 * i) ^ 2) // 2)
        return (
            remote(attn.at[0, :, mine_cols], attn.at[1, :, mine_cols], send2.at[0, i], recv2.at[0, i], at(1), head),
            remote(attn.at[0, :, mine_cols], attn.at[2, :, mine_cols], send2.at[1, i], recv2.at[1, i], at(2), head),
            remote(attn.at[2, :, peer_cols], attn.at[3, :, peer_cols], send2.at[2, i], recv2.at[2, i], at(1), head),
        )

    steps = [moves(i) for i in range(4)]

    def share(i):
        for core in range(2):
            for p, (_, dst) in enumerate(pieces(me)):
                arrived = remote(dst, dst, send1.at[0, p], recv1.at[i, core, p], me, core_peer)
                if i:
                    arrived.wait_recv()
                else:
                    @pl.when((c != x) | (core != c))
                    def _():
                        arrived.wait_recv()

        if i == 0:
            @pl.when(c == x)
            def _():
                for copy in local:
                    copy.wait()

        steps[i][1].start()
        steps[i][0].start()

    def forward(i):
        steps[i][1].wait_recv()
        steps[i][2].start()

    late = [g for g, (role, first, size) in enumerate(groups) if role and first >= early]

    def w_late(g):
        _, first, size = groups[g]
        return remote(
            w.at[:, pl.ds(first, size)], wpart.at[:, pl.ds(first, size)], wsem_s.at[g], wsem_r.at[g], at(4), head
        )

    def block_of(g):
        return 1 - mine if groups[g][0] else mine

    def span(g):
        role, first, size = groups[g]
        return pl.ds(role * wide + first, size)

    def inner(g):
        return pl.ds(groups[g][1], groups[g][2])

    def swap(g, r):
        return remote(
            d_send.at[r, :, span(g)], d_recv.at[r, :, span(g)], dsem_s.at[g, r], dsem_r.at[g, r], me, core_peer
        )

    def over_y(g, r):
        return remote(
            y_send.at[r, :, inner(g)], y_recv.at[r, :, inner(g)], ysem_s.at[g, r], ysem_r.at[g, r], me, y_peer
        )

    def target(g):
        return out.at[rows(c * half, half), pl.ds(pl.multiple_of(x * wide + groups[g][1], HD), groups[g][2])]

    def home(g, r):
        return remote(
            final.at[r, :, inner(g)], target(g), osem_s.at[g, r], osem_r.at[2 * x + c, g], at(r), 2 * y + zl
        )

    def home_here(g):
        return pltpu.make_async_copy(final.at[0, :, inner(g)], target(g), osem_l.at[g])

    def multiply(g, r):
        role, first, size = groups[g]
        weights = wpart if role else wown

        def one(t, carry):
            side = (1 - c) * (1 - t) + c * t
            value = jnp.dot(
                attn[r, rows(side * half, half), :], weights[:, pl.ds(first, size)], preferred_element_type=jnp.float32
            )

            @pl.when(t == 0)
            def _():
                d_send[r, :, span(g)] = value.astype(jnp.bfloat16)
                swap(g, r).start()

            @pl.when(t == 1)
            def _():
                part[r, :, span(g)] = value

            return carry

        lax.fori_loop(0, 2, one, 0)

    def add_core(g, r):
        swap(g, r).wait_recv()

        @pl.when(y == block_of(g))
        def _():
            part[r, :, span(g)] = part[r, :, span(g)] + d_recv[r, :, span(g)].astype(jnp.float32)

        @pl.when(y != block_of(g))
        def _():
            value = part[r, :, span(g)] + d_recv[r, :, span(g)].astype(jnp.float32)
            y_send[r, :, inner(g)] = value.astype(jnp.bfloat16)
            over_y(g, r).start()

    def finish(g, r):
        @pl.when(y == block_of(g))
        def _():
            over_y(g, r).wait_recv()
            value = part[r, :, span(g)] + y_recv[r, :, inner(g)].astype(jnp.float32)
            final[r, :, inner(g)] = value.astype(jnp.bfloat16)
            if r:
                home(g, r).start()
            else:
                @pl.when(zl != c)
                def _():
                    home(g, 0).start()

                @pl.when(zl == c)
                def _():
                    home_here(g).start()

    ready = [g for g in range(len(groups)) if g not in late]

    def shard(r):
        for i, g in enumerate(ready):
            multiply(g, r)
            if i:
                add_core(ready[i - 1], r)
        add_core(ready[-1], r)

    share(0)
    share(1)
    forward(0)
    share(2)
    forward(1)
    share(3)
    for g in late:
        w_late(g).start()
    forward(2)
    own_w.wait()
    got_w.wait()
    shard(0)
    forward(3)
    for r in range(1, 4):
        for i in range(4):
            steps[i][(None, 0, 1, 2)[r]].wait_recv() if r != 2 else None
        shard(r)
        for g in ready:
            finish(g, r - 1)
    units = [(g, r) for g in late for r in range(4)]
    pending = [(g, 3) for g in ready]
    for i, (g, r) in enumerate(units):
        if r == 0:
            w_late(g).wait_recv()
        multiply(g, r)
        if i:
            add_core(*units[i - 1])
            pending.append(units[i - 1])
        if i >= 3:
            finish(*pending.pop(0))
    add_core(*units[-1])
    for unit in pending + units[-1:]:
        finish(*unit)

    for k in range(1, n):
        for copy in back(k):
            copy.wait_send()

    @pl.when(c != x)
    def _():
        for copy in back(0):
            copy.wait_send()

    for copies in steps:
        for copy in copies:
            copy.wait_send()
    for g in late:
        w_late(g).wait_send()
    for g in range(len(groups)):
        for r in range(4):
            swap(g, r).wait_send()

            @pl.when(y != block_of(g))
            def _():
                over_y(g, r).wait_send()

            if r:
                @pl.when(y == block_of(g))
                def _():
                    home(g, r).wait_send()

        @pl.when((y == block_of(g)) & (zl != c))
        def _():
            home(g, 0).wait_send()

        @pl.when((y == block_of(g)) & (zl == c))
        def _():
            home_here(g).wait()

        for sx in range(2):
            for sc in range(2):
                piece = final.at[0, :, inner(g)]
                arrived = remote(piece, piece, osem_s.at[g, 0], osem_r.at[2 * sx + sc, g], me, core_peer)

                @pl.when((y == block_of(g)) & ((zl != c) | (sx != x) | (sc != c)))
                def _():
                    arrived.wait_recv()


def attend_kernel(odd_ref, count_ref, list_ref, qf, qs, kf, ks, vf, vs, of, os):
    odd = odd_ref[0]
    j = pl.program_id(0)
    factor = math.log2(math.e) / math.sqrt(HD)

    def scores(q, k):
        return lax.dot_general(q, k, (((1,), (1,)), ((), ())), preferred_element_type=jnp.float32)

    def fold(state, parts, vals):
        peak, total, accum = state
        top = parts[0]
        for s in parts[1:]:
            top = jnp.maximum(top, s)
        new_peak = jnp.maximum(peak, jnp.max(top, axis=1, keepdims=True))
        keep = jnp.exp2((peak - new_peak) * factor)
        total, accum = total * keep, accum * keep
        for s, v in zip(parts, vals):
            p = jnp.exp2((s - new_peak) * factor)
            for c in range(0, BLK, HD):
                total = total + p[:, c:c + HD]
            accum = accum + jnp.dot(p.astype(jnp.bfloat16), v, preferred_element_type=jnp.float32)
        return new_peak, total, accum

    def start():
        return (
            jnp.full((BLK, 1), NEG, jnp.float32),
            jnp.zeros((BLK, HD), jnp.float32),
            jnp.zeros((BLK, HD), jnp.float32),
        )

    def finish(state):
        _, total, accum = state
        return (accum / jnp.sum(total, axis=1, keepdims=True)).astype(jnp.bfloat16)

    def walk(block, streams):
        count = count_ref[block]

        def step(i, states):
            a = rows(list_ref[block, 2 * i] * BLK, BLK)
            b = rows(list_ref[block, 2 * i + 1] * BLK, BLK)
            bias = jnp.where(2 * i + 1 < count, 0.0, NEG).astype(jnp.float32)
            parts = [[scores(q, k[a, :]), scores(q, k[b, :]) + bias] for q, k, _ in streams]
            return tuple(
                fold(state, part, (v[a, :], v[b, :])) for state, part, (_, _, v) in zip(states, parts, streams)
            )

        return lax.fori_loop(0, (count + 1) // 2, step, tuple(start() for _ in streams))

    same, other = rows(odd * BLK, BLK), rows((1 - odd) * BLK, BLK)
    first, second = walk(2 * j + odd, [(qf[same, :], kf, vf), (qs[...], ks, vs)])
    of[same, :] = finish(first)
    os[...] = finish(second)
    (third,) = walk(2 * j + 1 - odd, [(qf[other, :], kf, vf)])
    of[other, :] = finish(third)


def body_spread(n, queries, keys, values, frame_of_block, pair_mask, w_out):
    tok, width = queries.shape
    count_blocks = pair_mask.shape[1]
    tokens = n * tok
    per = tok // BLK
    meta = jnp.concatenate([frame_of_block[:, None], pair_mask], axis=1)
    meta = jnp.pad(meta, ((0, 8 - per), (0, HD - 1 - count_blocks)))
    anyspace = pl.BlockSpec(memory_space=pl.ANY)
    big = jax.ShapeDtypeStruct((tokens, HD), queries.dtype)
    small = jax.ShapeDtypeStruct((tokens // 2, HD), queries.dtype)
    qf, qs, kf, ks, vf, vs, metas = pl.pallas_call(
        functools.partial(spread_kernel, n, tok),
        out_shape=[big, small, big, big, big, big, jax.ShapeDtypeStruct((8 * n, HD), jnp.int32)],
        in_specs=[anyspace] * 4,
        out_specs=[anyspace] * 7,
        scratch_shapes=[
            pltpu.VMEM((4, tok, HD), queries.dtype),
            pltpu.VMEM((tok // 2, HD), queries.dtype),
            pltpu.VMEM((8, HD), jnp.int32),
            pltpu.SemaphoreType.DMA((4, 2, 6)),
            pltpu.SemaphoreType.DMA((4, 2, 6)),
            pltpu.SemaphoreType.DMA((2, 6)),
            pltpu.SemaphoreType.DMA((4, 2)),
            pltpu.SemaphoreType.DMA((4, 2)),
        ],
        compiler_params=pltpu.CompilerParams(collective_id=0, has_side_effects=True),
        cost_estimate=pl.CostEstimate(flops=0, bytes_accessed=300_000_000, transcendentals=0),
        name="spread",
    )(queries, keys, values, meta)

    metas = metas.reshape(n, 8, HD)[:, :per].reshape(n * per, HD)
    frame, links = metas[:, 0], metas[:, 1:1 + count_blocks]
    allowed = (frame[None, :] <= frame[:, None]) & ((links == 1) | (frame[None, :] == frame[:, None]))
    place = jnp.cumsum(allowed.astype(jnp.int32), axis=1)
    count = place[:, -1]
    ids = jnp.arange(count_blocks, dtype=jnp.int32)
    hit = allowed[:, None, :] & (place[:, None, :] == ids[None, :, None] + 1)
    order = jnp.sum(jnp.where(hit, ids[None, None, :], 0), axis=2)
    odd = lax.rem(lax.axis_index("head"), 2).reshape(1).astype(jnp.int32)

    smem = pl.BlockSpec(memory_space=pltpu.SMEM)
    whole = pl.BlockSpec((tokens, HD), lambda j: (0, 0))
    two = pl.BlockSpec((2 * BLK, HD), lambda j: (j, 0))
    one = pl.BlockSpec((BLK, HD), lambda j: (j, 0))
    of, os = pl.pallas_call(
        attend_kernel,
        grid=(tokens // (2 * BLK),),
        out_shape=[big, small],
        in_specs=[smem, smem, smem, two, one, whole, whole, whole, whole],
        out_specs=[two, one],
        compiler_params=pltpu.CompilerParams(vmem_limit_bytes=60 * 1024 * 1024),
        cost_estimate=pl.CostEstimate(flops=20_000_000_000, bytes_accessed=8_000_000, transcendentals=20_000_000),
        name="attend",
    )(odd, count, order, qf, qs, kf, ks, vf, vs)

    deep, wide = w_out.shape
    early = wide // 2
    w_early, _ = lax.optimization_barrier((w_out[:, :early], kf))
    w_got = lax.ppermute(w_early, "seq", [(i, (i + n // 2) % n) for i in range(n)])
    groups = [(0, 0, early), (0, early, wide - early), (1, 0, early)]
    groups += [(1, early, wide - early - HD), (1, wide - HD, HD)]
    count = len(groups)
    dma = pltpu.SemaphoreType.DMA
    return pl.pallas_call(
        functools.partial(project_kernel, n, tok, groups),
        out_shape=jax.ShapeDtypeStruct((tok, 2 * wide), queries.dtype),
        in_specs=[anyspace] * 4,
        out_specs=anyspace,
        scratch_shapes=[
            pltpu.VMEM((4, tok, width), queries.dtype),
            pltpu.VMEM((deep, wide), queries.dtype),
            pltpu.VMEM((deep, wide), queries.dtype),
            pltpu.VMEM((4, tok // 2, 2 * wide), jnp.float32),
            pltpu.VMEM((4, tok // 2, 2 * wide), queries.dtype),
            pltpu.VMEM((4, tok // 2, 2 * wide), queries.dtype),
            pltpu.VMEM((4, tok // 2, wide), queries.dtype),
            pltpu.VMEM((4, tok // 2, wide), queries.dtype),
            pltpu.VMEM((4, tok // 2, wide), queries.dtype),
            dma((n, 2)), dma((4, 2, 2)), dma((4,)), dma((3, 4)), dma((3, 4)), dma((count,)), dma((count,)),
            dma((count, 4)), dma((count, 4)), dma((count, 4)), dma((count, 4)),
            dma((count, 4)), dma((4, count)), dma((count,)),
        ],
        compiler_params=pltpu.CompilerParams(
            collective_id=1, has_side_effects=True, vmem_limit_bytes=58 * 1024 * 1024
        ),
        cost_estimate=pl.CostEstimate(flops=10_000_000_000, bytes_accessed=30_000_000, transcendentals=0),
        name="project",
    )(of, os, w_out, w_got)


def body(n, groups, queries, keys, values, frame_of_block, pair_mask, w_out):
    heads_here = queries.shape[1] // HD
    fits = n == 8 and groups == 4 and 2 * heads_here == 3 * n and queries.shape[0] == 2 * BLK
    if fits:
        return body_spread(n, queries, keys, values, frame_of_block, pair_mask, w_out)
    return body_gather(queries, keys, values, frame_of_block, pair_mask, w_out)


def solution(mesh):
    placed = (
        P("seq", "head"),
        P("seq", "head"),
        P("seq", "head"),
        P("seq"),
        P("seq", None),
        P("head", "seq"),
    )
    return jax.shard_map(
        functools.partial(body, mesh.shape["seq"], mesh.shape["head"]), mesh=mesh, in_specs=placed, out_specs=P("seq", "head"), check_vma=False
    )
```

```python
import functools
import math

import jax
import jax.numpy as jnp
from jax import lax
from jax.experimental import pallas as pl
from jax.experimental.pallas import tpu as pltpu
from jax.sharding import PartitionSpec as P

HD = 128
BLK = 256
NEG = -1e30


def body_gather(queries, keys, values, frame_of_block, pair_mask, w_out):
    tok = queries.shape[0]
    heads_here = queries.shape[1] // HD
    count_blocks = pair_mask.shape[1]
    scale = 1.0 / math.sqrt(HD)
    key_span = 512
    q_heads = queries.reshape(tok, heads_here, HD)
    q_frame = jnp.repeat(frame_of_block, BLK)
    mask_rows = jnp.repeat(pair_mask.astype(jnp.float32), BLK, axis=0)
    block_ids = jnp.arange(count_blocks, dtype=jnp.int32)

    def update(state, k_rows, v_rows, allowed):
        peak, total, accum = state
        k_heads = k_rows.reshape(k_rows.shape[0], heads_here, HD)
        v_heads = v_rows.reshape(v_rows.shape[0], heads_here, HD)
        score = (
            jnp.einsum("qhd,khd->hqk", q_heads, k_heads, preferred_element_type=jnp.float32) * scale
        )
        score = jnp.where(allowed[None], score, -1e30)
        new_peak = jnp.maximum(peak, jnp.max(score, axis=2))
        weight = jnp.where(allowed[None], jnp.exp(score - new_peak[:, :, None]), 0.0)
        factor = jnp.exp(peak - new_peak)
        new_total = total * factor + jnp.sum(weight, axis=2)
        added = jnp.einsum(
            "hqk,khd->qhd", weight.astype(jnp.bfloat16), v_heads, preferred_element_type=jnp.float32
        )
        new_accum = accum * factor.T[:, :, None] + added
        return (new_peak, new_total, new_accum)

    def attend_block(state, k_rows, v_rows, k_frame, start):
        count = k_rows.shape[0]
        k_block = (start + jnp.arange(count, dtype=jnp.int32)) // BLK
        one_hot = (block_ids[:, None] == k_block[None, :]).astype(jnp.float32)
        link = jnp.dot(mask_rows, one_hot, preferred_element_type=jnp.float32)
        same = k_frame[None, :] == q_frame[:, None]
        allowed = (k_frame[None, :] <= q_frame[:, None]) & ((link > 0.5) | same)
        return update(state, k_rows, v_rows, allowed)

    initial = (
        jnp.full((heads_here, tok), -1e30, jnp.float32),
        jnp.zeros((heads_here, tok), jnp.float32),
        jnp.zeros((tok, heads_here, HD), jnp.float32),
    )
    k_frame_local = jnp.repeat(frame_of_block, BLK)
    k_rows = lax.all_gather(keys, "seq", axis=0, tiled=True)
    v_rows = lax.all_gather(values, "seq", axis=0, tiled=True)
    k_frame = lax.all_gather(k_frame_local, "seq", axis=0, tiled=True)
    count = k_rows.shape[0]

    def step(index, inner):
        offset = (index * key_span).astype(jnp.int32)
        return attend_block(
            inner,
            lax.dynamic_slice_in_dim(k_rows, offset, key_span, 0),
            lax.dynamic_slice_in_dim(v_rows, offset, key_span, 0),
            lax.dynamic_slice_in_dim(k_frame, offset, key_span, 0),
            offset,
        )

    state = lax.fori_loop(0, count // key_span, step, initial)
    peak, total, accum = state
    attn = (accum / total.T[:, :, None]).reshape(tok, heads_here * HD).astype(jnp.bfloat16)
    terms = jnp.dot(
        attn, lax.all_gather(w_out, "seq", axis=1, tiled=True), preferred_element_type=jnp.float32
    )
    return lax.psum_scatter(terms.astype(jnp.bfloat16), "head", scatter_dimension=1, tiled=True)


def flip(bit, value):
    return 1 - value if bit else value


def greet(plane):
    barrier = pltpu.get_barrier_semaphore()
    for seq, head in plane:
        pl.semaphore_signal(
            barrier, inc=1, device_id={"seq": seq, "head": head}, device_id_type=pl.DeviceIdType.MESH
        )
    return lambda: pl.semaphore_wait(barrier, len(plane))


def remote(src, dst, send, recv, seq, head):
    return pltpu.make_async_remote_copy(
        src_ref=src, dst_ref=dst, send_sem=send, recv_sem=recv,
        device_id={"seq": seq, "head": head}, device_id_type=pl.DeviceIdType.MESH,
    )


def cols(head):
    return pl.ds(pl.multiple_of(head * HD, HD), HD)


def rows(start, size):
    return pl.ds(pl.multiple_of(start, size), size)


def spread_kernel(
    n, tok, q, k, v, meta, w, qf, qs, kf, ks, vf, vs, metas, w_early,
    hold, hold_half, hold_meta, hold_w, here_w, send, recv, here, fsem_s, fsem_r,
):
    me, head = lax.axis_index("seq"), lax.axis_index("head")
    half = tok // 2
    x, zl, zh = lax.rem(me, 2), lax.rem(me // 2, 2), me // 4
    c, y = lax.rem(head, 2), head // 2
    other = 2 * y + 1 - c
    cross = x * (1 - c) + (1 - x) * c

    def layer(i):
        return 2 * flip(i & 2, zh) + flip(i & 1, zl)

    def pieces(i, far):
        pair, core = layer(i), flip(far, c)
        own, shared = cols(3 * pair + 2 * core), cols(3 * pair + 1)
        full = rows(me * tok, tok)
        return [
            (q.at[:, own], qf.at[full]),
            (k.at[:, own], kf.at[full]),
            (v.at[:, own], vf.at[full]),
            (q.at[rows(core * half, half), shared], qs.at[rows(me * half, half)]),
            (v.at[:, shared], vs.at[full]) if far else (k.at[:, shared], ks.at[full]),
            (meta, metas.at[rows(me * 8, 8)]),
        ]

    def out_copies(i, far):
        return [
            remote(src, dst, send.at[i, far, p], recv.at[i, cross, p], 2 * layer(i) + c, 2 * y + flip(far, c))
            for p, (src, dst) in enumerate(pieces(i, far))
        ]

    def from_row(i, side):
        return 2 * layer(i) + flip(side, x)

    def forward(i, side, keys):
        piece = (ks if keys else vs).at[rows(from_row(i, side) * tok, tok)]
        return remote(piece, piece, fsem_s.at[i, side], fsem_r.at[i, side], me, other)

    greet([(2 * layer(i) + flip(side, x), 2 * y + core) for i in range(4) for side in range(2) for core in range(2)
           if i or side] + [(me, other)])()
    w_in = pltpu.make_async_copy(w.at[:, pl.ds(0, w_early.shape[1])], hold_w, here_w.at[0])
    w_out = pltpu.make_async_copy(hold_w, w_early, here_w.at[1])
    w_in.start()
    for i in (2, 3, 1):
        for far in range(2):
            for copy in out_copies(i, far):
                copy.start()
    for copy in out_copies(0, 1):
        copy.start()

    @pl.when(x != c)
    def _():
        for copy in out_copies(0, 0):
            copy.start()

    @pl.when(x == c)
    def _():
        mine = pieces(0, 0)
        via = [hold.at[0], hold.at[1], hold.at[2], hold_half, hold.at[3], hold_meta]
        ins = [pltpu.make_async_copy(src, mid, here.at[0, p]) for p, ((src, _), mid) in enumerate(zip(mine, via))]
        outs = [pltpu.make_async_copy(mid, dst, here.at[1, p]) for p, ((_, dst), mid) in enumerate(zip(mine, via))]
        for one in ins:
            one.start()
        for one, two in zip(ins, outs):
            one.wait()
            two.start()
        for two in outs:
            two.wait()

    w_in.wait()
    w_out.start()
    w_out.wait()

    def arrive(i, side):
        for p, (_, dst) in enumerate(pieces(i, 0)):
            remote(dst, dst, send.at[i, 0, p], recv.at[i, side, p], me, other).wait_recv()

    for i in (0, 1, 2, 3):
        for side in range(2):
            if i or side:
                arrive(i, side)
            else:
                @pl.when(x != c)
                def _():
                    arrive(0, 0)

            for keys in (True, False):
                @pl.when((x == c) == keys)
                def _():
                    forward(i, side, keys).start()

    for i in range(4):
        for side in range(2):
            for keys in (True, False):
                @pl.when((x == c) == keys)
                def _():
                    forward(i, side, keys).wait_send()
                    forward(i, side, not keys).wait_recv()

        for far in range(2):
            if i or far:
                for copy in out_copies(i, far):
                    copy.wait_send()
            else:
                @pl.when(x != c)
                def _():
                    for copy in out_copies(0, 0):
                        copy.wait_send()


def project_kernel(
    n, tok, groups, of, os, w, wgot, out, attn, wown, wpart, part, d_send, d_recv, y_send, y_recv, final,
    send1, recv1, here, send2, recv2, wsem_s, wsem_r, dsem_s, dsem_r, ysem_s, ysem_r, osem_s, osem_r, osem_l,
):
    me, head = lax.axis_index("seq"), lax.axis_index("head")
    half = tok // 2
    wide = w.shape[1]
    early = wgot.shape[1]
    c, y = lax.rem(head, 2), head // 2
    x, zl, mine = lax.rem(me, 2), lax.rem(me // 2, 2), me // 4
    core_peer = 2 * y + 1 - c
    y_peer = 2 * (1 - y) + c

    def at(k):
        return 4 * flip(k & 4, mine) + 2 * flip(k & 2, zl) + flip(k & 1, x)

    met = greet([(at(k), 2 * y + core) for k in range(1, n) for core in range(2)] + [(me, core_peer), (me, y_peer)])
    own_w = pltpu.make_async_copy(w, wown, here.at[2])
    own_w.start()
    got_w = pltpu.make_async_copy(wgot, wpart.at[:, pl.ds(0, early)], here.at[3])
    got_w.start()
    met()

    own, shared = cols(3 * (me // 2) + 2 * c), cols(3 * (me // 2) + 1)

    def pieces(to):
        return [
            (of.at[rows(to * tok, tok)], attn.at[0, :, own]),
            (os.at[rows(to * half, half)], attn.at[0, rows(c * half, half), shared]),
        ]

    def back(k):
        return [
            remote(src, dst, send1.at[k, p], recv1.at[k // 2, c, p], at(k), 2 * y + x)
            for p, (src, dst) in enumerate(pieces(at(k)))
        ]

    local = [pltpu.make_async_copy(src, dst, here.at[p]) for p, (src, dst) in enumerate(pieces(me))]
    for k in range(1, n):
        for copy in back(k):
            copy.start()

    @pl.when(c != x)
    def _():
        for copy in back(0):
            copy.start()

    @pl.when(c == x)
    def _():
        for copy in local:
            copy.start()

    def chunk(at_pair):
        return pl.ds(pl.multiple_of(3 * HD * at_pair, HD), 3 * HD)

    def moves(i):
        mine_cols = chunk(at(2 * i) // 2)
        peer_cols = chunk(at((2 * i) ^ 2) // 2)
        return (
            remote(attn.at[0, :, mine_cols], attn.at[1, :, mine_cols], send2.at[0, i], recv2.at[0, i], at(1), head),
            remote(attn.at[0, :, mine_cols], attn.at[2, :, mine_cols], send2.at[1, i], recv2.at[1, i], at(2), head),
            remote(attn.at[2, :, peer_cols], attn.at[3, :, peer_cols], send2.at[2, i], recv2.at[2, i], at(1), head),
        )

    steps = [moves(i) for i in range(4)]

    def share(i):
        for core in range(2):
            for p, (_, dst) in enumerate(pieces(me)):
                arrived = remote(dst, dst, send1.at[0, p], recv1.at[i, core, p], me, core_peer)
                if i:
                    arrived.wait_recv()
                else:
                    @pl.when((c != x) | (core != c))
                    def _():
                        arrived.wait_recv()

        if i == 0:
            @pl.when(c == x)
            def _():
                for copy in local:
                    copy.wait()

        steps[i][1].start()
        steps[i][0].start()

    def forward(i):
        steps[i][1].wait_recv()
        steps[i][2].start()

    late = [g for g, (role, first, size) in enumerate(groups) if role and first >= early]

    def w_late(g):
        _, first, size = groups[g]
        return remote(
            w.at[:, pl.ds(first, size)], wpart.at[:, pl.ds(first, size)], wsem_s.at[g], wsem_r.at[g], at(4), head
        )

    def block_of(g):
        return 1 - mine if groups[g][0] else mine

    def span(g):
        role, first, size = groups[g]
        return pl.ds(role * wide + first, size)

    def inner(g):
        return pl.ds(groups[g][1], groups[g][2])

    def swap(g, r):
        return remote(
            d_send.at[r, :, span(g)], d_recv.at[r, :, span(g)], dsem_s.at[g, r], dsem_r.at[g, r], me, core_peer
        )

    def over_y(g, r):
        return remote(
            y_send.at[r, :, inner(g)], y_recv.at[r, :, inner(g)], ysem_s.at[g, r], ysem_r.at[g, r], me, y_peer
        )

    def target(g):
        return out.at[rows(c * half, half), pl.ds(pl.multiple_of(x * wide + groups[g][1], HD), groups[g][2])]

    def home(g, r):
        return remote(
            final.at[r, :, inner(g)], target(g), osem_s.at[g, r], osem_r.at[2 * x + c, g], at(r), 2 * y + zl
        )

    def home_here(g):
        return pltpu.make_async_copy(final.at[0, :, inner(g)], target(g), osem_l.at[g])

    def multiply(g, r):
        role, first, size = groups[g]
        weights = wpart if role else wown

        def one(t, carry):
            side = (1 - c) * (1 - t) + c * t
            value = jnp.dot(
                attn[r, rows(side * half, half), :], weights[:, pl.ds(first, size)], preferred_element_type=jnp.float32
            )

            @pl.when(t == 0)
            def _():
                d_send[r, :, span(g)] = value.astype(jnp.bfloat16)
                swap(g, r).start()

            @pl.when(t == 1)
            def _():
                part[r, :, span(g)] = value

            return carry

        lax.fori_loop(0, 2, one, 0)

    def add_core(g, r):
        swap(g, r).wait_recv()

        @pl.when(y == block_of(g))
        def _():
            part[r, :, span(g)] = part[r, :, span(g)] + d_recv[r, :, span(g)].astype(jnp.float32)

        @pl.when(y != block_of(g))
        def _():
            value = part[r, :, span(g)] + d_recv[r, :, span(g)].astype(jnp.float32)
            y_send[r, :, inner(g)] = value.astype(jnp.bfloat16)
            over_y(g, r).start()

    def finish(g, r):
        @pl.when(y == block_of(g))
        def _():
            over_y(g, r).wait_recv()
            value = part[r, :, span(g)] + y_recv[r, :, inner(g)].astype(jnp.float32)
            final[r, :, inner(g)] = value.astype(jnp.bfloat16)
            if r:
                home(g, r).start()
            else:
                @pl.when(zl != c)
                def _():
                    home(g, 0).start()

                @pl.when(zl == c)
                def _():
                    home_here(g).start()

    ready = [g for g in range(len(groups)) if g not in late]

    def shard(r):
        for i, g in enumerate(ready):
            multiply(g, r)
            if i:
                add_core(ready[i - 1], r)
        add_core(ready[-1], r)

    share(0)
    share(1)
    forward(0)
    share(2)
    forward(1)
    share(3)
    for g in late:
        w_late(g).start()
    forward(2)
    own_w.wait()
    got_w.wait()
    shard(0)
    forward(3)
    for r in range(1, 4):
        for i in range(4):
            steps[i][(None, 0, 1, 2)[r]].wait_recv() if r != 2 else None
        shard(r)
        for g in ready:
            finish(g, r - 1)
    units = [(g, r) for g in late for r in range(4)]
    pending = [(g, 3) for g in ready]
    for i, (g, r) in enumerate(units):
        if r == 0:
            w_late(g).wait_recv()
        multiply(g, r)
        if i:
            add_core(*units[i - 1])
            pending.append(units[i - 1])
        if i >= 3:
            finish(*pending.pop(0))
    add_core(*units[-1])
    for unit in pending + units[-1:]:
        finish(*unit)

    for k in range(1, n):
        for copy in back(k):
            copy.wait_send()

    @pl.when(c != x)
    def _():
        for copy in back(0):
            copy.wait_send()

    for copies in steps:
        for copy in copies:
            copy.wait_send()
    for g in late:
        w_late(g).wait_send()
    for g in range(len(groups)):
        for r in range(4):
            swap(g, r).wait_send()

            @pl.when(y != block_of(g))
            def _():
                over_y(g, r).wait_send()

            if r:
                @pl.when(y == block_of(g))
                def _():
                    home(g, r).wait_send()

        @pl.when((y == block_of(g)) & (zl != c))
        def _():
            home(g, 0).wait_send()

        @pl.when((y == block_of(g)) & (zl == c))
        def _():
            home_here(g).wait()

        for sx in range(2):
            for sc in range(2):
                piece = final.at[0, :, inner(g)]
                arrived = remote(piece, piece, osem_s.at[g, 0], osem_r.at[2 * sx + sc, g], me, core_peer)

                @pl.when((y == block_of(g)) & ((zl != c) | (sx != x) | (sc != c)))
                def _():
                    arrived.wait_recv()


def attend_kernel(odd_ref, count_ref, list_ref, qf, qs, kf, ks, vf, vs, of, os):
    odd = odd_ref[0]
    j = pl.program_id(0)
    factor = math.log2(math.e) / math.sqrt(HD)

    def scores(q, k):
        return lax.dot_general(q, k, (((1,), (1,)), ((), ())), preferred_element_type=jnp.float32)

    def fold(state, parts, vals):
        peak, total, accum = state
        top = parts[0]
        for s in parts[1:]:
            top = jnp.maximum(top, s)
        new_peak = jnp.maximum(peak, jnp.max(top, axis=1, keepdims=True))
        keep = jnp.exp2((peak - new_peak) * factor)
        total, accum = total * keep, accum * keep
        for s, v in zip(parts, vals):
            p = jnp.exp2((s - new_peak) * factor)
            for c in range(0, BLK, HD):
                total = total + p[:, c:c + HD]
            accum = accum + jnp.dot(p.astype(jnp.bfloat16), v, preferred_element_type=jnp.float32)
        return new_peak, total, accum

    def start():
        return (
            jnp.full((BLK, 1), NEG, jnp.float32),
            jnp.zeros((BLK, HD), jnp.float32),
            jnp.zeros((BLK, HD), jnp.float32),
        )

    def finish(state):
        _, total, accum = state
        return (accum / jnp.sum(total, axis=1, keepdims=True)).astype(jnp.bfloat16)

    def walk(block, streams):
        count = count_ref[block]

        def step(i, states):
            a = rows(list_ref[block, 2 * i] * BLK, BLK)
            b = rows(list_ref[block, 2 * i + 1] * BLK, BLK)
            bias = jnp.where(2 * i + 1 < count, 0.0, NEG).astype(jnp.float32)
            parts = [[scores(q, k[a, :]), scores(q, k[b, :]) + bias] for q, k, _ in streams]
            return tuple(
                fold(state, part, (v[a, :], v[b, :])) for state, part, (_, _, v) in zip(states, parts, streams)
            )

        return lax.fori_loop(0, (count + 1) // 2, step, tuple(start() for _ in streams))

    same, other = rows(odd * BLK, BLK), rows((1 - odd) * BLK, BLK)
    first, second = walk(2 * j + odd, [(qf[same, :], kf, vf), (qs[...], ks, vs)])
    of[same, :] = finish(first)
    os[...] = finish(second)
    (third,) = walk(2 * j + 1 - odd, [(qf[other, :], kf, vf)])
    of[other, :] = finish(third)


def body_spread(n, queries, keys, values, frame_of_block, pair_mask, w_out):
    tok, width = queries.shape
    count_blocks = pair_mask.shape[1]
    tokens = n * tok
    per = tok // BLK
    meta = jnp.concatenate([frame_of_block[:, None], pair_mask], axis=1)
    meta = jnp.pad(meta, ((0, 8 - per), (0, HD - 1 - count_blocks)))
    anyspace = pl.BlockSpec(memory_space=pl.ANY)
    big = jax.ShapeDtypeStruct((tokens, HD), queries.dtype)
    small = jax.ShapeDtypeStruct((tokens // 2, HD), queries.dtype)
    deep, wide = w_out.shape
    early = wide // 2
    qf, qs, kf, ks, vf, vs, metas, w_early = pl.pallas_call(
        functools.partial(spread_kernel, n, tok),
        out_shape=[big, small, big, big, big, big, jax.ShapeDtypeStruct((8 * n, HD), jnp.int32),
                   jax.ShapeDtypeStruct((deep, early), w_out.dtype)],
        in_specs=[anyspace] * 5,
        out_specs=[anyspace] * 8,
        scratch_shapes=[
            pltpu.VMEM((4, tok, HD), queries.dtype),
            pltpu.VMEM((tok // 2, HD), queries.dtype),
            pltpu.VMEM((8, HD), jnp.int32),
            pltpu.VMEM((deep, early), w_out.dtype),
            pltpu.SemaphoreType.DMA((2,)),
            pltpu.SemaphoreType.DMA((4, 2, 6)),
            pltpu.SemaphoreType.DMA((4, 2, 6)),
            pltpu.SemaphoreType.DMA((2, 6)),
            pltpu.SemaphoreType.DMA((4, 2)),
            pltpu.SemaphoreType.DMA((4, 2)),
        ],
        compiler_params=pltpu.CompilerParams(collective_id=0, has_side_effects=True),
        cost_estimate=pl.CostEstimate(flops=0, bytes_accessed=300_000_000, transcendentals=0),
        name="spread",
    )(queries, keys, values, meta, w_out)

    metas = metas.reshape(n, 8, HD)[:, :per].reshape(n * per, HD)
    frame, links = metas[:, 0], metas[:, 1:1 + count_blocks]
    allowed = (frame[None, :] <= frame[:, None]) & ((links == 1) | (frame[None, :] == frame[:, None]))
    place = jnp.cumsum(allowed.astype(jnp.int32), axis=1)
    count = place[:, -1]
    ids = jnp.arange(count_blocks, dtype=jnp.int32)
    hit = allowed[:, None, :] & (place[:, None, :] == ids[None, :, None] + 1)
    order = jnp.sum(jnp.where(hit, ids[None, None, :], 0), axis=2)
    odd = lax.rem(lax.axis_index("head"), 2).reshape(1).astype(jnp.int32)

    smem = pl.BlockSpec(memory_space=pltpu.SMEM)
    whole = pl.BlockSpec((tokens, HD), lambda j: (0, 0))
    two = pl.BlockSpec((2 * BLK, HD), lambda j: (j, 0))
    one = pl.BlockSpec((BLK, HD), lambda j: (j, 0))
    of, os = pl.pallas_call(
        attend_kernel,
        grid=(tokens // (2 * BLK),),
        out_shape=[big, small],
        in_specs=[smem, smem, smem, two, one, whole, whole, whole, whole],
        out_specs=[two, one],
        compiler_params=pltpu.CompilerParams(vmem_limit_bytes=60 * 1024 * 1024),
        cost_estimate=pl.CostEstimate(flops=20_000_000_000, bytes_accessed=8_000_000, transcendentals=20_000_000),
        name="attend",
    )(odd, count, order, qf, qs, kf, ks, vf, vs)

    w_got = lax.ppermute(w_early, "seq", [(i, (i + n // 2) % n) for i in range(n)])
    groups = [(0, 0, early), (0, early, wide - early), (1, 0, early)]
    groups += [(1, early, wide - early - HD), (1, wide - HD, HD)]
    count = len(groups)
    dma = pltpu.SemaphoreType.DMA
    return pl.pallas_call(
        functools.partial(project_kernel, n, tok, groups),
        out_shape=jax.ShapeDtypeStruct((tok, 2 * wide), queries.dtype),
        in_specs=[anyspace] * 4,
        out_specs=anyspace,
        scratch_shapes=[
            pltpu.VMEM((4, tok, width), queries.dtype),
            pltpu.VMEM((deep, wide), queries.dtype),
            pltpu.VMEM((deep, wide), queries.dtype),
            pltpu.VMEM((4, tok // 2, 2 * wide), jnp.float32),
            pltpu.VMEM((4, tok // 2, 2 * wide), queries.dtype),
            pltpu.VMEM((4, tok // 2, 2 * wide), queries.dtype),
            pltpu.VMEM((4, tok // 2, wide), queries.dtype),
            pltpu.VMEM((4, tok // 2, wide), queries.dtype),
            pltpu.VMEM((4, tok // 2, wide), queries.dtype),
            dma((n, 2)), dma((4, 2, 2)), dma((4,)), dma((3, 4)), dma((3, 4)), dma((count,)), dma((count,)),
            dma((count, 4)), dma((count, 4)), dma((count, 4)), dma((count, 4)),
            dma((count, 4)), dma((4, count)), dma((count,)),
        ],
        compiler_params=pltpu.CompilerParams(
            collective_id=1, has_side_effects=True, vmem_limit_bytes=58 * 1024 * 1024
        ),
        cost_estimate=pl.CostEstimate(flops=10_000_000_000, bytes_accessed=30_000_000, transcendentals=0),
        name="project",
    )(of, os, w_out, w_got)


def body(n, groups, queries, keys, values, frame_of_block, pair_mask, w_out):
    heads_here = queries.shape[1] // HD
    fits = n == 8 and groups == 4 and 2 * heads_here == 3 * n and queries.shape[0] == 2 * BLK
    if fits:
        return body_spread(n, queries, keys, values, frame_of_block, pair_mask, w_out)
    return body_gather(queries, keys, values, frame_of_block, pair_mask, w_out)


def solution(mesh):
    placed = (
        P("seq", "head"),
        P("seq", "head"),
        P("seq", "head"),
        P("seq"),
        P("seq", None),
        P("head", "seq"),
    )
    return jax.shard_map(
        functools.partial(body, mesh.shape["seq"], mesh.shape["head"]), mesh=mesh, in_specs=placed, out_specs=P("seq", "head"), check_vma=False
    )
```

```python
import functools
import math

import jax
import jax.numpy as jnp
from jax import lax
from jax.experimental import pallas as pl
from jax.experimental.pallas import tpu as pltpu
from jax.sharding import PartitionSpec as P

HD = 128
BLK = 256
NEG = -1e30


def body_gather(queries, keys, values, frame_of_block, pair_mask, w_out):
    tok = queries.shape[0]
    heads_here = queries.shape[1] // HD
    count_blocks = pair_mask.shape[1]
    scale = 1.0 / math.sqrt(HD)
    key_span = 512
    q_heads = queries.reshape(tok, heads_here, HD)
    q_frame = jnp.repeat(frame_of_block, BLK)
    mask_rows = jnp.repeat(pair_mask.astype(jnp.float32), BLK, axis=0)
    block_ids = jnp.arange(count_blocks, dtype=jnp.int32)

    def update(state, k_rows, v_rows, allowed):
        peak, total, accum = state
        k_heads = k_rows.reshape(k_rows.shape[0], heads_here, HD)
        v_heads = v_rows.reshape(v_rows.shape[0], heads_here, HD)
        score = (
            jnp.einsum("qhd,khd->hqk", q_heads, k_heads, preferred_element_type=jnp.float32) * scale
        )
        score = jnp.where(allowed[None], score, -1e30)
        new_peak = jnp.maximum(peak, jnp.max(score, axis=2))
        weight = jnp.where(allowed[None], jnp.exp(score - new_peak[:, :, None]), 0.0)
        factor = jnp.exp(peak - new_peak)
        new_total = total * factor + jnp.sum(weight, axis=2)
        added = jnp.einsum(
            "hqk,khd->qhd", weight.astype(jnp.bfloat16), v_heads, preferred_element_type=jnp.float32
        )
        new_accum = accum * factor.T[:, :, None] + added
        return (new_peak, new_total, new_accum)

    def attend_block(state, k_rows, v_rows, k_frame, start):
        count = k_rows.shape[0]
        k_block = (start + jnp.arange(count, dtype=jnp.int32)) // BLK
        one_hot = (block_ids[:, None] == k_block[None, :]).astype(jnp.float32)
        link = jnp.dot(mask_rows, one_hot, preferred_element_type=jnp.float32)
        same = k_frame[None, :] == q_frame[:, None]
        allowed = (k_frame[None, :] <= q_frame[:, None]) & ((link > 0.5) | same)
        return update(state, k_rows, v_rows, allowed)

    initial = (
        jnp.full((heads_here, tok), -1e30, jnp.float32),
        jnp.zeros((heads_here, tok), jnp.float32),
        jnp.zeros((tok, heads_here, HD), jnp.float32),
    )
    k_frame_local = jnp.repeat(frame_of_block, BLK)
    k_rows = lax.all_gather(keys, "seq", axis=0, tiled=True)
    v_rows = lax.all_gather(values, "seq", axis=0, tiled=True)
    k_frame = lax.all_gather(k_frame_local, "seq", axis=0, tiled=True)
    count = k_rows.shape[0]

    def step(index, inner):
        offset = (index * key_span).astype(jnp.int32)
        return attend_block(
            inner,
            lax.dynamic_slice_in_dim(k_rows, offset, key_span, 0),
            lax.dynamic_slice_in_dim(v_rows, offset, key_span, 0),
            lax.dynamic_slice_in_dim(k_frame, offset, key_span, 0),
            offset,
        )

    state = lax.fori_loop(0, count // key_span, step, initial)
    peak, total, accum = state
    attn = (accum / total.T[:, :, None]).reshape(tok, heads_here * HD).astype(jnp.bfloat16)
    terms = jnp.dot(
        attn, lax.all_gather(w_out, "seq", axis=1, tiled=True), preferred_element_type=jnp.float32
    )
    return lax.psum_scatter(terms.astype(jnp.bfloat16), "head", scatter_dimension=1, tiled=True)


def flip(bit, value):
    return 1 - value if bit else value


def greet(plane):
    barrier = pltpu.get_barrier_semaphore()
    for seq, head in plane:
        pl.semaphore_signal(
            barrier, inc=1, device_id={"seq": seq, "head": head}, device_id_type=pl.DeviceIdType.MESH
        )
    return lambda: pl.semaphore_wait(barrier, len(plane))


def remote(src, dst, send, recv, seq, head):
    return pltpu.make_async_remote_copy(
        src_ref=src, dst_ref=dst, send_sem=send, recv_sem=recv,
        device_id={"seq": seq, "head": head}, device_id_type=pl.DeviceIdType.MESH,
    )


def cols(head):
    return pl.ds(pl.multiple_of(head * HD, HD), HD)


def rows(start, size):
    return pl.ds(pl.multiple_of(start, size), size)


def spread_kernel(
    n, tok, q, k, v, meta, w, qf, qs, kf, ks, vf, vs, metas, w_early,
    hold, hold_half, hold_meta, hold_w, here_w, send, recv, here, fsem_s, fsem_r,
):
    me, head = lax.axis_index("seq"), lax.axis_index("head")
    half = tok // 2
    x, zl, zh = lax.rem(me, 2), lax.rem(me // 2, 2), me // 4
    c, y = lax.rem(head, 2), head // 2
    other = 2 * y + 1 - c
    cross = x * (1 - c) + (1 - x) * c

    def layer(i):
        return 2 * flip(i & 2, zh) + flip(i & 1, zl)

    def pieces(i, far):
        pair, core = layer(i), flip(far, c)
        own, shared = cols(3 * pair + 2 * core), cols(3 * pair + 1)
        full = rows(me * tok, tok)
        return [
            (q.at[:, own], qf.at[full]),
            (k.at[:, own], kf.at[full]),
            (v.at[:, own], vf.at[full]),
            (q.at[rows(core * half, half), shared], qs.at[rows(me * half, half)]),
            (v.at[:, shared], vs.at[full]) if far else (k.at[:, shared], ks.at[full]),
            (meta, metas.at[rows(me * 8, 8)]),
        ]

    def out_copies(i, far):
        return [
            remote(src, dst, send.at[i, far, p], recv.at[i, cross, p], 2 * layer(i) + c, 2 * y + flip(far, c))
            for p, (src, dst) in enumerate(pieces(i, far))
        ]

    def from_row(i, side):
        return 2 * layer(i) + flip(side, x)

    def forward(i, side, keys):
        piece = (ks if keys else vs).at[rows(from_row(i, side) * tok, tok)]
        return remote(piece, piece, fsem_s.at[i, side], fsem_r.at[i, side], me, other)

    greet([(2 * layer(i) + flip(side, x), 2 * y + core) for i in range(4) for side in range(2) for core in range(2)
           if i or side] + [(me, other)])()
    w_in = pltpu.make_async_copy(w.at[:, pl.ds(0, w_early.shape[1])], hold_w, here_w.at[0])
    w_out = pltpu.make_async_copy(hold_w, w_early, here_w.at[1])
    w_in.start()
    for i in (2, 3, 1):
        for far in range(2):
            for copy in out_copies(i, far):
                copy.start()
    for copy in out_copies(0, 1):
        copy.start()

    @pl.when(x != c)
    def _():
        for copy in out_copies(0, 0):
            copy.start()

    @pl.when(x == c)
    def _():
        mine = pieces(0, 0)
        via = [hold.at[0], hold.at[1], hold.at[2], hold_half, hold.at[3], hold_meta]
        ins = [pltpu.make_async_copy(src, mid, here.at[0, p]) for p, ((src, _), mid) in enumerate(zip(mine, via))]
        outs = [pltpu.make_async_copy(mid, dst, here.at[1, p]) for p, ((_, dst), mid) in enumerate(zip(mine, via))]
        for one in ins:
            one.start()
        for one, two in zip(ins, outs):
            one.wait()
            two.start()
        for two in outs:
            two.wait()

    w_in.wait()
    w_out.start()
    w_out.wait()

    def arrive(i, side):
        for p, (_, dst) in enumerate(pieces(i, 0)):
            remote(dst, dst, send.at[i, 0, p], recv.at[i, side, p], me, other).wait_recv()

    for i in (0, 1, 2, 3):
        for side in range(2):
            if i or side:
                arrive(i, side)
            else:
                @pl.when(x != c)
                def _():
                    arrive(0, 0)

            for keys in (True, False):
                @pl.when((x == c) == keys)
                def _():
                    forward(i, side, keys).start()

    for i in range(4):
        for side in range(2):
            for keys in (True, False):
                @pl.when((x == c) == keys)
                def _():
                    forward(i, side, keys).wait_send()
                    forward(i, side, not keys).wait_recv()

        for far in range(2):
            if i or far:
                for copy in out_copies(i, far):
                    copy.wait_send()
            else:
                @pl.when(x != c)
                def _():
                    for copy in out_copies(0, 0):
                        copy.wait_send()


def project_kernel(
    n, tok, groups, of, os, w, wgot, out, attn, wown, wpart, part, d_send, d_recv, y_send, y_recv, final,
    send1, recv1, here, send2, recv2, wsem_s, wsem_r, dsem_s, dsem_r, ysem_s, ysem_r, osem_s, osem_r, osem_l,
):
    me, head = lax.axis_index("seq"), lax.axis_index("head")
    half = tok // 2
    wide = w.shape[1]
    early = wgot.shape[1]
    c, y = lax.rem(head, 2), head // 2
    x, zl, mine = lax.rem(me, 2), lax.rem(me // 2, 2), me // 4
    core_peer = 2 * y + 1 - c
    y_peer = 2 * (1 - y) + c

    def at(k):
        return 4 * flip(k & 4, mine) + 2 * flip(k & 2, zl) + flip(k & 1, x)

    met = greet([(at(k), 2 * y + core) for k in range(1, n) for core in range(2)] + [(me, core_peer), (me, y_peer)])
    own_w = pltpu.make_async_copy(w, wown, here.at[2])
    own_w.start()
    got_w = pltpu.make_async_copy(wgot, wpart.at[:, pl.ds(0, early)], here.at[3])
    got_w.start()
    met()

    own, shared = cols(3 * (me // 2) + 2 * c), cols(3 * (me // 2) + 1)

    def pieces(to):
        return [
            (of.at[rows(to * tok, tok)], attn.at[0, :, own]),
            (os.at[rows(to * half, half)], attn.at[0, rows(c * half, half), shared]),
        ]

    def back(k):
        return [
            remote(src, dst, send1.at[k, p], recv1.at[k // 2, c, p], at(k), 2 * y + x)
            for p, (src, dst) in enumerate(pieces(at(k)))
        ]

    local = [pltpu.make_async_copy(src, dst, here.at[p]) for p, (src, dst) in enumerate(pieces(me))]
    for k in range(1, n):
        for copy in back(k):
            copy.start()

    @pl.when(c != x)
    def _():
        for copy in back(0):
            copy.start()

    @pl.when(c == x)
    def _():
        for copy in local:
            copy.start()

    def chunk(at_pair):
        return pl.ds(pl.multiple_of(3 * HD * at_pair, HD), 3 * HD)

    def moves(i):
        mine_cols = chunk(at(2 * i) // 2)
        peer_cols = chunk(at((2 * i) ^ 2) // 2)
        return (
            remote(attn.at[0, :, mine_cols], attn.at[1, :, mine_cols], send2.at[0, i], recv2.at[0, i], at(1), head),
            remote(attn.at[0, :, mine_cols], attn.at[2, :, mine_cols], send2.at[1, i], recv2.at[1, i], at(2), head),
            remote(attn.at[2, :, peer_cols], attn.at[3, :, peer_cols], send2.at[2, i], recv2.at[2, i], at(1), head),
        )

    steps = [moves(i) for i in range(4)]

    def share(i):
        for core in range(2):
            for p, (_, dst) in enumerate(pieces(me)):
                arrived = remote(dst, dst, send1.at[0, p], recv1.at[i, core, p], me, core_peer)
                if i:
                    arrived.wait_recv()
                else:
                    @pl.when((c != x) | (core != c))
                    def _():
                        arrived.wait_recv()

        if i == 0:
            @pl.when(c == x)
            def _():
                for copy in local:
                    copy.wait()

        steps[i][1].start()
        steps[i][0].start()

    def forward(i):
        steps[i][1].wait_recv()
        steps[i][2].start()

    late = [g for g, (role, first, size) in enumerate(groups) if role and first >= early]

    def w_late(g):
        _, first, size = groups[g]
        return remote(
            w.at[:, pl.ds(first, size)], wpart.at[:, pl.ds(first, size)], wsem_s.at[g], wsem_r.at[g], at(4), head
        )

    def block_of(g):
        return 1 - mine if groups[g][0] else mine

    def span(g):
        role, first, size = groups[g]
        return pl.ds(role * wide + first, size)

    def inner(g):
        return pl.ds(groups[g][1], groups[g][2])

    def swap(g, r):
        return remote(
            d_send.at[r, :, span(g)], d_recv.at[r, :, span(g)], dsem_s.at[g, r], dsem_r.at[g, r], me, core_peer
        )

    def over_y(g, r):
        return remote(
            y_send.at[r, :, inner(g)], y_recv.at[r, :, inner(g)], ysem_s.at[g, r], ysem_r.at[g, r], me, y_peer
        )

    def target(g):
        return out.at[rows(c * half, half), pl.ds(pl.multiple_of(x * wide + groups[g][1], HD), groups[g][2])]

    def home(g, r):
        return remote(
            final.at[r, :, inner(g)], target(g), osem_s.at[g, r], osem_r.at[2 * x + c, g], at(r), 2 * y + zl
        )

    def home_here(g):
        return pltpu.make_async_copy(final.at[0, :, inner(g)], target(g), osem_l.at[g])

    def multiply(g, r):
        role, first, size = groups[g]
        weights = wpart if role else wown

        def one(t, carry):
            side = (1 - c) * (1 - t) + c * t
            value = jnp.dot(
                attn[r, rows(side * half, half), :], weights[:, pl.ds(first, size)], preferred_element_type=jnp.float32
            )

            @pl.when(t == 0)
            def _():
                d_send[r, :, span(g)] = value.astype(jnp.bfloat16)
                swap(g, r).start()

            @pl.when(t == 1)
            def _():
                part[r, :, span(g)] = value

            return carry

        lax.fori_loop(0, 2, one, 0)

    def add_core(g, r):
        swap(g, r).wait_recv()

        @pl.when(y == block_of(g))
        def _():
            part[r, :, span(g)] = part[r, :, span(g)] + d_recv[r, :, span(g)].astype(jnp.float32)

        @pl.when(y != block_of(g))
        def _():
            value = part[r, :, span(g)] + d_recv[r, :, span(g)].astype(jnp.float32)
            y_send[r, :, inner(g)] = value.astype(jnp.bfloat16)
            over_y(g, r).start()

    def finish(g, r):
        @pl.when(y == block_of(g))
        def _():
            over_y(g, r).wait_recv()
            value = part[r, :, span(g)] + y_recv[r, :, inner(g)].astype(jnp.float32)
            final[r, :, inner(g)] = value.astype(jnp.bfloat16)
            if r:
                home(g, r).start()
            else:
                @pl.when(zl != c)
                def _():
                    home(g, 0).start()

                @pl.when(zl == c)
                def _():
                    home_here(g).start()

    ready = [g for g in range(len(groups)) if g not in late]

    def shard(r):
        for i, g in enumerate(ready):
            multiply(g, r)
            if i:
                add_core(ready[i - 1], r)
        add_core(ready[-1], r)

    share(0)
    share(1)
    forward(0)
    share(2)
    forward(1)
    share(3)
    for g in late:
        w_late(g).start()
    forward(2)
    own_w.wait()
    got_w.wait()
    shard(0)
    forward(3)
    for r in range(1, 4):
        for i in range(4):
            steps[i][(None, 0, 1, 2)[r]].wait_recv() if r != 2 else None
        shard(r)
        if r > 1:
            for g in ready:
                finish(g, r - 2)
    units = [(g, r) for g in late for r in range(4)]
    pending = [(g, r) for r in (2, 3) for g in ready]
    for i, (g, r) in enumerate(units):
        if r == 0:
            w_late(g).wait_recv()
        multiply(g, r)
        if i:
            add_core(*units[i - 1])
            pending.append(units[i - 1])
        if i >= 1:
            finish(*pending.pop(0))
        if i in (2, 4, 6):
            finish(*pending.pop(0))
    add_core(*units[-1])
    for unit in pending + units[-1:]:
        finish(*unit)

    for k in range(1, n):
        for copy in back(k):
            copy.wait_send()

    @pl.when(c != x)
    def _():
        for copy in back(0):
            copy.wait_send()

    for copies in steps:
        for copy in copies:
            copy.wait_send()
    for g in late:
        w_late(g).wait_send()
    for g in range(len(groups)):
        for r in range(4):
            swap(g, r).wait_send()

            @pl.when(y != block_of(g))
            def _():
                over_y(g, r).wait_send()

            if r:
                @pl.when(y == block_of(g))
                def _():
                    home(g, r).wait_send()

        @pl.when((y == block_of(g)) & (zl != c))
        def _():
            home(g, 0).wait_send()

        @pl.when((y == block_of(g)) & (zl == c))
        def _():
            home_here(g).wait()

        for sx in range(2):
            for sc in range(2):
                piece = final.at[0, :, inner(g)]
                arrived = remote(piece, piece, osem_s.at[g, 0], osem_r.at[2 * sx + sc, g], me, core_peer)

                @pl.when((y == block_of(g)) & ((zl != c) | (sx != x) | (sc != c)))
                def _():
                    arrived.wait_recv()


def attend_kernel(odd_ref, count_ref, list_ref, qf, qs, kf, ks, vf, vs, of, os):
    odd = odd_ref[0]
    j = pl.program_id(0)
    factor = math.log2(math.e) / math.sqrt(HD)

    def scores(q, k):
        return lax.dot_general(q, k, (((1,), (1,)), ((), ())), preferred_element_type=jnp.float32)

    def fold(state, parts, vals):
        peak, total, accum = state
        top = parts[0]
        for s in parts[1:]:
            top = jnp.maximum(top, s)
        new_peak = jnp.maximum(peak, jnp.max(top, axis=1, keepdims=True))
        keep = jnp.exp2((peak - new_peak) * factor)
        total, accum = total * keep, accum * keep
        for s, v in zip(parts, vals):
            p = jnp.exp2((s - new_peak) * factor)
            for c in range(0, BLK, HD):
                total = total + p[:, c:c + HD]
            accum = accum + jnp.dot(p.astype(jnp.bfloat16), v, preferred_element_type=jnp.float32)
        return new_peak, total, accum

    def start():
        return (
            jnp.full((BLK, 1), NEG, jnp.float32),
            jnp.zeros((BLK, HD), jnp.float32),
            jnp.zeros((BLK, HD), jnp.float32),
        )

    def finish(state):
        _, total, accum = state
        return (accum / jnp.sum(total, axis=1, keepdims=True)).astype(jnp.bfloat16)

    def walk(block, streams):
        count = count_ref[block]

        def step(i, states):
            a = rows(list_ref[block, 2 * i] * BLK, BLK)
            b = rows(list_ref[block, 2 * i + 1] * BLK, BLK)
            bias = jnp.where(2 * i + 1 < count, 0.0, NEG).astype(jnp.float32)
            parts = [[scores(q, k[a, :]), scores(q, k[b, :]) + bias] for q, k, _ in streams]
            return tuple(
                fold(state, part, (v[a, :], v[b, :])) for state, part, (_, _, v) in zip(states, parts, streams)
            )

        return lax.fori_loop(0, (count + 1) // 2, step, tuple(start() for _ in streams))

    same, other = rows(odd * BLK, BLK), rows((1 - odd) * BLK, BLK)
    first, second = walk(2 * j + odd, [(qf[same, :], kf, vf), (qs[...], ks, vs)])
    of[same, :] = finish(first)
    os[...] = finish(second)
    (third,) = walk(2 * j + 1 - odd, [(qf[other, :], kf, vf)])
    of[other, :] = finish(third)


def body_spread(n, queries, keys, values, frame_of_block, pair_mask, w_out):
    tok, width = queries.shape
    count_blocks = pair_mask.shape[1]
    tokens = n * tok
    per = tok // BLK
    meta = jnp.concatenate([frame_of_block[:, None], pair_mask], axis=1)
    meta = jnp.pad(meta, ((0, 8 - per), (0, HD - 1 - count_blocks)))
    anyspace = pl.BlockSpec(memory_space=pl.ANY)
    big = jax.ShapeDtypeStruct((tokens, HD), queries.dtype)
    small = jax.ShapeDtypeStruct((tokens // 2, HD), queries.dtype)
    deep, wide = w_out.shape
    early = wide // 2
    qf, qs, kf, ks, vf, vs, metas, w_early = pl.pallas_call(
        functools.partial(spread_kernel, n, tok),
        out_shape=[big, small, big, big, big, big, jax.ShapeDtypeStruct((8 * n, HD), jnp.int32),
                   jax.ShapeDtypeStruct((deep, early), w_out.dtype)],
        in_specs=[anyspace] * 5,
        out_specs=[anyspace] * 8,
        scratch_shapes=[
            pltpu.VMEM((4, tok, HD), queries.dtype),
            pltpu.VMEM((tok // 2, HD), queries.dtype),
            pltpu.VMEM((8, HD), jnp.int32),
            pltpu.VMEM((deep, early), w_out.dtype),
            pltpu.SemaphoreType.DMA((2,)),
            pltpu.SemaphoreType.DMA((4, 2, 6)),
            pltpu.SemaphoreType.DMA((4, 2, 6)),
            pltpu.SemaphoreType.DMA((2, 6)),
            pltpu.SemaphoreType.DMA((4, 2)),
            pltpu.SemaphoreType.DMA((4, 2)),
        ],
        compiler_params=pltpu.CompilerParams(collective_id=0, has_side_effects=True),
        cost_estimate=pl.CostEstimate(flops=0, bytes_accessed=300_000_000, transcendentals=0),
        name="spread",
    )(queries, keys, values, meta, w_out)

    metas = metas.reshape(n, 8, HD)[:, :per].reshape(n * per, HD)
    frame, links = metas[:, 0], metas[:, 1:1 + count_blocks]
    allowed = (frame[None, :] <= frame[:, None]) & ((links == 1) | (frame[None, :] == frame[:, None]))
    place = jnp.cumsum(allowed.astype(jnp.int32), axis=1)
    count = place[:, -1]
    ids = jnp.arange(count_blocks, dtype=jnp.int32)
    hit = allowed[:, None, :] & (place[:, None, :] == ids[None, :, None] + 1)
    order = jnp.sum(jnp.where(hit, ids[None, None, :], 0), axis=2)
    odd = lax.rem(lax.axis_index("head"), 2).reshape(1).astype(jnp.int32)

    smem = pl.BlockSpec(memory_space=pltpu.SMEM)
    whole = pl.BlockSpec((tokens, HD), lambda j: (0, 0))
    two = pl.BlockSpec((2 * BLK, HD), lambda j: (j, 0))
    one = pl.BlockSpec((BLK, HD), lambda j: (j, 0))
    of, os = pl.pallas_call(
        attend_kernel,
        grid=(tokens // (2 * BLK),),
        out_shape=[big, small],
        in_specs=[smem, smem, smem, two, one, whole, whole, whole, whole],
        out_specs=[two, one],
        compiler_params=pltpu.CompilerParams(vmem_limit_bytes=60 * 1024 * 1024),
        cost_estimate=pl.CostEstimate(flops=20_000_000_000, bytes_accessed=8_000_000, transcendentals=20_000_000),
        name="attend",
    )(odd, count, order, qf, qs, kf, ks, vf, vs)

    w_got = lax.ppermute(w_early, "seq", [(i, (i + n // 2) % n) for i in range(n)])
    groups = [(0, 0, early), (0, early, wide - early), (1, 0, early)]
    groups += [(1, early, wide - early - HD), (1, wide - HD, HD)]
    count = len(groups)
    dma = pltpu.SemaphoreType.DMA
    return pl.pallas_call(
        functools.partial(project_kernel, n, tok, groups),
        out_shape=jax.ShapeDtypeStruct((tok, 2 * wide), queries.dtype),
        in_specs=[anyspace] * 4,
        out_specs=anyspace,
        scratch_shapes=[
            pltpu.VMEM((4, tok, width), queries.dtype),
            pltpu.VMEM((deep, wide), queries.dtype),
            pltpu.VMEM((deep, wide), queries.dtype),
            pltpu.VMEM((4, tok // 2, 2 * wide), jnp.float32),
            pltpu.VMEM((4, tok // 2, 2 * wide), queries.dtype),
            pltpu.VMEM((4, tok // 2, 2 * wide), queries.dtype),
            pltpu.VMEM((4, tok // 2, wide), queries.dtype),
            pltpu.VMEM((4, tok // 2, wide), queries.dtype),
            pltpu.VMEM((4, tok // 2, wide), queries.dtype),
            dma((n, 2)), dma((4, 2, 2)), dma((4,)), dma((3, 4)), dma((3, 4)), dma((count,)), dma((count,)),
            dma((count, 4)), dma((count, 4)), dma((count, 4)), dma((count, 4)),
            dma((count, 4)), dma((4, count)), dma((count,)),
        ],
        compiler_params=pltpu.CompilerParams(
            collective_id=1, has_side_effects=True, vmem_limit_bytes=58 * 1024 * 1024
        ),
        cost_estimate=pl.CostEstimate(flops=10_000_000_000, bytes_accessed=30_000_000, transcendentals=0),
        name="project",
    )(of, os, w_out, w_got)


def body(n, groups, queries, keys, values, frame_of_block, pair_mask, w_out):
    heads_here = queries.shape[1] // HD
    fits = n == 8 and groups == 4 and 2 * heads_here == 3 * n and queries.shape[0] == 2 * BLK
    if fits:
        return body_spread(n, queries, keys, values, frame_of_block, pair_mask, w_out)
    return body_gather(queries, keys, values, frame_of_block, pair_mask, w_out)


def solution(mesh):
    placed = (
        P("seq", "head"),
        P("seq", "head"),
        P("seq", "head"),
        P("seq"),
        P("seq", None),
        P("head", "seq"),
    )
    return jax.shard_map(
        functools.partial(body, mesh.shape["seq"], mesh.shape["head"]), mesh=mesh, in_specs=placed, out_specs=P("seq", "head"), check_vma=False
    )
```
